128 devices in a mesh: band: 32 (over x, y, core), grid: 4 (over z).
Axes of the slice: x: 4, y: 4, z: 4, core: 2. Of those that a mesh axis runs over, the one named last changes fastest.
Arguments:
- orbitals: bfloat16 [256, 128, 128, 128], P('band', None, 'grid'), may hold values from -0.375 to 0.375
- occupations: float32 [256], P('band'), may hold values from 0 to 2
- rho_in: float32 [128, 128, 128], P('band', 'grid'), may hold values from 0.5 to 1.5
- hist_in: float32 [7, 128, 128, 128], P(None, 'band', 'grid'), may hold values from 0.5 to 1.5
- hist_res: float32 [7, 128, 128, 128], P(None, 'band', 'grid'), may hold values from -10 to 10
Outputs:
- rho_next: float32 [128, 128, 128], P('band', 'grid')
- v_hartree: float32 [128, 128, 128], P('band', 'grid')
The draws below stay inside these ranges and needn't reach their ends.
All inputs are finite; a program needn't handle non-finite values.
Results may differ from the reference program's by a relative error of at most 0.0003.
Values sent between devices are 32-bit elements; how exact they have to be, the bound alone decides.
A program may use at most 64 MiB of HBM per device.

```python
import jax
import jax.numpy as jnp
from jax import lax

N = 128
HIST = 7
BANDS = 256


def draw_hist_res(key, part):
    base_key = jax.random.fold_in(key, 17)
    key_common, key_own, key_scale = jax.random.split(base_key, 3)
    common = jnp.clip(jax.random.normal(key_common, (N, N, N), jnp.float32), -5.0, 5.0)
    shared = 0.5
    own_part = jnp.clip(jax.random.normal(key_own, (HIST, N, N, N), jnp.float32), -5.0, 5.0)
    scales = jnp.exp(jax.random.uniform(key_scale, (HIST,), jnp.float32, -2.302585, 0.0))
    return scales[:, None, None, None] * (shared * common[None] + own_part)


def level_of(own_key, extent, cuts, least, high):
    def one(axis_at, blocks):
        steps = jax.random.uniform(jax.random.fold_in(jax.random.fold_in(own_key, 6), axis_at), (blocks,), jnp.float32, least / len(cuts), high / len(cuts))
        return jnp.repeat(jnp.exp(steps), extent[axis_at] // blocks).reshape((-1,) + (1,) * (len(extent) - axis_at - 1))

    factor_of = one(*cuts[0])
    for cut in cuts[1:]:
        factor_of = factor_of * one(*cut)
    return factor_of


def bell_draw(key, extent, deviation, limit, pieces=(), kind=jnp.bfloat16):
    drawn = deviation * jax.random.normal(key, extent, jnp.float32)
    if pieces:
        drawn = drawn * level_of(key, extent, pieces, -0.22, 0.18)
    return jnp.clip(drawn, -limit, limit).astype(kind)


def setup_inputs(seed: int = 0) -> dict:
    seeds = jax.random.split(jax.random.key(seed), 6)
    orbitals = bell_draw(seeds[0], (BANDS, N, N, N), BANDS ** -0.5, 0.375, ((0, 32), (2, 4)))
    occupations = jnp.clip(2.0 * jax.random.uniform(seeds[1], (BANDS,), jnp.float32) ** level_of(seeds[1], (BANDS,), ((0, 32),), -0.2, 0.2), 0.0, 2.0)
    rho_in = jnp.clip(0.5 + 1.0 * jax.random.uniform(seeds[2], (N, N, N), jnp.float32) ** level_of(seeds[2], (N, N, N), ((0, 32), (1, 4)), -0.2, 0.2), 0.5, 1.5)
    hist_in = jnp.clip(0.5 + 1.0 * jax.random.uniform(seeds[3], (HIST, N, N, N), jnp.float32) ** level_of(seeds[3], (HIST, N, N, N), ((1, 32), (2, 4)), -0.2, 0.2), 0.5, 1.5)
    hist_res = draw_hist_res(jax.random.fold_in(seeds[5], 71), 0)
    return dict(orbitals=orbitals, occupations=occupations, rho_in=rho_in, hist_in=hist_in, hist_res=hist_res)


beta_mix = 0.5
spacing = 0.2

def coulomb_kernel(length):
    positions = jnp.arange(length, dtype=jnp.int32)
    freq_all = jnp.where(positions < length // 2, positions, positions - length)
    square_all = freq_all * freq_all
    squared_sum = square_all[:, None, None] + square_all[None, :, None] + square_all[None, None, :]
    cell_len = length * spacing
    floored = jnp.maximum(squared_sum, 1).astype(jnp.float32)
    values_all = cell_len * cell_len / jnp.pi / floored
    return jnp.where(squared_sum > 0, values_all, jnp.zeros_like(values_all)).astype(jnp.float32)

def reference(orbitals, occupations, rho_in, hist_in, hist_res):

    def add_band(summed, band_pair):
        orbital, weight = band_pair
        amplitude = orbital.astype(jnp.float32)
        return (summed + weight * amplitude * amplitude, None)
    rho_out, _ = lax.scan(add_band, jnp.zeros((N, N, N), jnp.float32), (orbitals, occupations))
    res_new = rho_out - rho_in
    residuals = jnp.concatenate([hist_res, res_new[None]], axis=0)
    inputs = jnp.concatenate([hist_in, rho_in[None]], axis=0)
    flat_res = residuals.reshape(HIST + 1, N * N * N)
    gram_matrix = jnp.dot(flat_res.astype(jnp.float32), flat_res.T.astype(jnp.float32), precision=lax.Precision.HIGHEST, preferred_element_type=jnp.float32) / (N * N * N)
    factor = jnp.linalg.cholesky(gram_matrix)
    solved = jax.scipy.linalg.cho_solve((factor, True), jnp.ones((HIST + 1,), jnp.float32))
    weights = solved / jnp.sum(solved)
    trials = inputs + beta_mix * residuals
    rho_next = jnp.tensordot(weights, trials, axes=1, precision=lax.Precision.HIGHEST)
    spectrum = jnp.fft.fftn(rho_next)
    v_hartree = jnp.real(jnp.fft.ifftn(spectrum * coulomb_kernel(N))).astype(jnp.float32)
    return (rho_next, v_hartree)
```

```python
import functools

import jax
import jax.numpy as jnp
import numpy as np
from jax import lax
from jax.experimental import pallas as pl
from jax.experimental.pallas import tpu as pltpu
from jax.sharding import Mesh
from jax.sharding import PartitionSpec as P

LOGICAL = pl.DeviceIdType.LOGICAL
BAND = ("x", "y", "c")
N = 128
HIST = 7
CHUNKS = 16
beta_mix = 0.5
spacing = 0.2
f32 = jnp.float32
bf16 = jnp.bfloat16


def tables():
    k = np.arange(N)
    angle = 2.0 * np.pi * ((k[:, None] * k[None, :]) % N) / N
    basis = (np.cos(angle) + np.sin(angle)) / np.sqrt(N)
    order = (4 * np.arange(32)[None, :] + np.arange(4)[:, None]).reshape(-1)
    parts = []
    for table in (basis, basis[:, order], basis[order, :]):
        high = table.astype(jnp.bfloat16)
        low = (table - high.astype(np.float64)).astype(jnp.bfloat16)
        parts += [high, low]
    return jnp.asarray(np.stack(parts))


def halves(value):
    high = value.astype(bf16)
    return high, (value - high.astype(f32)).astype(bf16)


def product(left, right, dims):
    dot = functools.partial(
        lax.dot_general, dimension_numbers=(dims, ((), ())), preferred_element_type=f32
    )
    return dot(left[0], right[0]) + (dot(left[0], right[1]) + dot(left[1], right[0]))


def partner_ids(x, y, c, z):
    plane = {(i, j): ((x + i) % 4) * 32 + ((y + j) % 4) * 8 for i in range(4) for j in range(4)}
    rest = {(i, j): ((c + i) % 2) * 4 + (z + j) % 4 for i in range(2) for j in range(4)}
    slot_plane = {(i, j): ((x + i) % 4) * 8 + ((y + j) % 4) * 2 for i in range(4) for j in range(4)}
    slot_rest = {(i, j): ((c + i) % 2) + ((z + j) % 4) * 32 for i in range(2) for j in range(4)}
    moves = [(a, b, d, e) for a in range(4) for b in range(4) for d in range(2) for e in range(4)][1:]

    def hops(m):
        return sum((0, 1, 2, 1)[m[i]] for i in (0, 1, 3))

    moves.sort(key=lambda m: -hops(m))
    return [
        (plane[m[:2]] + rest[m[2:]], slot_plane[m[:2]] + slot_rest[m[2:]], m) for m in moves
    ]


def kernel(
    orb, occ, rin_h, hin_h, hres_h, tab_h, rho_h, v_h,
    orb_v, rin, hin, hres, tab, part, crecv, r1, r2, r3, r4,
    wide, grow, grecv, xsend, xrecv, vsend, vrecv, rho_v, v_v,
    load_sem, in_sem, out_sem, c_send, c_recv, rs_send, rs_recv, a_send, a_recv,
):
    x, y, c, z = (lax.axis_index(a) for a in ("x", "y", "c", "z"))

    def place(px, py, pc, pz):
        return px * 32 + py * 8 + pc * 4 + pz

    me = place(x, y, c, z)
    band = x * 8 + y * 2 + c
    my_slot = z * 32 + band
    others = partner_ids(x, y, c, z)

    barrier = pltpu.get_barrier_semaphore()
    near = [t for t, _, m in others if sum(v > 0 for v in m) == 1]
    for t in near:
        pl.semaphore_signal(barrier, inc=1, device_id=t, device_id_type=LOGICAL)

    def load(chunk):
        rows = pl.ds(chunk * 8, 8)
        return pltpu.make_async_copy(orb.at[:, rows], orb_v.at[:, rows], load_sem.at[chunk])

    for chunk in range(CHUNKS):
        load(chunk).start()
    inputs = [(tab_h, tab), (rin_h, rin), (hres_h, hres), (hin_h, hin)]
    for i, (a, b) in enumerate(inputs):
        pltpu.make_async_copy(a, b, in_sem.at[i]).start()

    weights_occ = [occ[k] for k in range(8)]

    @pl.loop(0, CHUNKS)
    def _(chunk):
        load(chunk).wait()
        for row in range(8):
            total = None
            for k in range(8):
                value = orb_v[k, chunk * 8 + row].astype(f32)
                term = weights_occ[k] * (value * value)
                total = term if total is None else total + term
            part[chunk // 4, chunk % 4, row // 4, row % 4] = total

    pl.semaphore_wait(barrier, len(near))

    def c_copy(s):
        return pltpu.make_async_remote_copy(
            src_ref=part.at[:, :, 1 - c, s], dst_ref=crecv.at[:, :, s],
            send_sem=c_send.at[s], recv_sem=c_recv.at[s],
            device_id=place(x, y, 1 - c, z), device_id_type=LOGICAL,
        )

    for s in (0, 2, 1, 3):
        c_copy(s).start()

    flip = {
        "x": {1: x + 1 - 2 * (x % 2), 2: (x + 2) % 4, 3: 3 - x},
        "y": {1: y + 1 - 2 * (y % 2), 2: (y + 2) % 4, 3: 3 - y},
    }
    mine = {"x": x, "y": y}
    orders = {0: ("x", "y", 1), 1: ("x", "y", 3), 2: ("y", "x", 1), 3: ("y", "x", 3)}

    def dev(axis, e):
        if axis == "x":
            return place(flip["x"][e], y, c, z)
        return place(x, flip["y"][e], c, z)

    def rows_of(axis, index, s):
        if axis == "x":
            return part.at[index, :, c, s]
        return part.at[:, index, c, s]

    def block_of(axis, index, s):
        if axis == "x":
            return part.at[index, y, c, s]
        return part.at[x, index, c, s]

    def steps(s):
        first, second, e1 = orders[s]
        e2 = 4 - e1
        slot = s * 6

        def remote(src, dst, sem, to):
            return pltpu.make_async_remote_copy(
                src_ref=src, dst_ref=dst, send_sem=rs_send.at[slot + sem],
                recv_sem=rs_recv.at[slot + sem], device_id=to, device_id_type=LOGICAL,
            )

        one = [
            (remote(rows_of(first, flip[first][e1], s), r1.at[s, 0], 0, dev(first, e1)),
             rows_of(first, mine[first], s), r1.at[s, 0]),
            (remote(rows_of(first, flip[first][2], s), r1.at[s, 1], 1, dev(first, e1)),
             rows_of(first, flip[first][e2], s), r1.at[s, 1]),
        ]
        two = [
            (remote(rows_of(first, flip[first][e2], s), r2.at[s], 2, dev(first, e2)),
             rows_of(first, mine[first], s), r2.at[s]),
        ]
        three = [
            (remote(block_of(second, flip[second][e1], s), r3.at[s, 0], 3, dev(second, e1)),
             block_of(second, mine[second], s), r3.at[s, 0]),
            (remote(block_of(second, flip[second][2], s), r3.at[s, 1], 4, dev(second, e1)),
             block_of(second, flip[second][e2], s), r3.at[s, 1]),
        ]
        four = [
            (remote(block_of(second, flip[second][e2], s), r4.at[s], 5, dev(second, e2)),
             block_of(second, mine[second], s), r4.at[s]),
        ]
        return [one, two, three, four]

    plan = {s: steps(s) for s in range(4)}
    for s in (0, 2, 1, 3):
        c_copy(s).wait_recv()
        own = part.at[:, :, c, s]
        own[...] = own[...] + crecv[:, :, s]
        for copy, _, _ in plan[s][0]:
            copy.start()

    for i, (a, b) in enumerate(inputs):
        pltpu.make_async_copy(a, b, in_sem.at[i]).wait()

    lane = lax.broadcasted_iota(jnp.int32, (8, N), 1)
    sub = lax.broadcasted_iota(jnp.int32, (8, N), 0)

    def fold(value):
        return jnp.sum(value.reshape(16, 8, N), axis=0)

    def products(i, field, amount):
        rows = jnp.zeros((8, N), f32)
        for j in range(amount):
            line = jnp.sum(fold(field * hres[j]), axis=0, keepdims=True)
            rows = jnp.where(sub == j, line, rows)
        return rows

    def placed(i, rows):
        total = jnp.sum(rows, axis=1, keepdims=True)
        spots = (lane == 8 * i + sub) | (lane == 8 * sub + i)
        return jnp.sum(jnp.where(spots & (sub <= i), total, 0.0), axis=0, keepdims=True)

    row = jnp.zeros((1, N), f32)
    for i in range(HIST):
        row = row + placed(i, products(i, hres[i], i + 1))

    wide[...] = jnp.zeros_like(wide)
    for half in range(2):
        for g in range(4):
            for a in range(4):
                wide[half, pl.ds(g * 128 + a * 32, 32), pl.ds(a * 128, 128)] = tab[
                    half, pl.ds(g * 32, 32), :
                ]

    for step in range(4):
        for s in (0, 2, 1, 3):
            for copy, into, came in plan[s][step]:
                copy.wait_recv()
                into[...] = into[...] + came[...]
            if step < 3:
                for copy, _, _ in plan[s][step + 1]:
                    copy.start()

    rho_out = part.at[x, y, c]
    new = rho_out[...].reshape(N, N) - rin[...]
    rows = products(7, new, HIST)
    line = jnp.sum(fold(new * new), axis=0, keepdims=True)
    rows = jnp.where(sub == 7, line, rows)
    row = row + placed(7, rows)
    grow[...] = row

    def exchange(source, target, sem):
        copies = []
        for t, slot, _ in others:
            copies.append(pltpu.make_async_remote_copy(
                src_ref=source(t, slot), dst_ref=target,
                send_sem=a_send.at[sem], recv_sem=a_recv.at[sem],
                device_id=t, device_id_type=LOGICAL,
            ))
        for copy in copies:
            copy.start()

    def arrived(buffer, sem):
        pltpu.make_async_copy(buffer.at[pl.ds(0, 127)], buffer.at[pl.ds(0, 127)], a_recv.at[sem]).wait()

    def sent(buffer, sem):
        pltpu.make_async_copy(buffer.at[pl.ds(0, 127)], buffer.at[pl.ds(0, 127)], a_send.at[sem]).wait()

    exchange(lambda t, slot: grow, grecv.at[pl.ds(me, 1)], 0)
    grecv[pl.ds(me, 1)] = row
    arrived(grecv, 0)
    flat = jnp.sum(grecv[...], axis=0, keepdims=True) * (1.0 / (N * N * N))
    matrix = jnp.zeros((8, N), f32)
    for i in range(8):
        shifted = flat if i == 0 else pltpu.roll(flat, N - 8 * i, 1)
        matrix = jnp.where(sub == i, shifted, matrix)
    matrix = jnp.where(lane < 8, matrix, jnp.where(lane == 8, 1.0, 0.0))
    for k in range(8):
        pivot_row = matrix[k : k + 1, :]
        column = jnp.sum(jnp.where(lane == k, matrix, 0.0), axis=1, keepdims=True)
        pivot = column[k : k + 1, :]
        matrix = jnp.where(sub == k, matrix, matrix - (column / pivot) * pivot_row)
    diagonal = jnp.sum(jnp.where(lane == sub, matrix, 0.0), axis=1, keepdims=True)
    right = jnp.sum(jnp.where(lane == 8, matrix, 0.0), axis=1, keepdims=True)
    solved = right / diagonal
    weights = solved / jnp.sum(solved, axis=0, keepdims=True)

    rho = weights[7:8, :] * (rin[...] + beta_mix * new)
    for m in range(HIST):
        rho = rho + weights[m : m + 1, :] * (hin[m] + beta_mix * hres[m])
    rho_v[...] = rho
    out_rho = pltpu.make_async_copy(rho_v, rho_h, out_sem.at[0])
    out_rho.start()

    basis = (tab[0], tab[1])
    xsend[...] = product(basis, halves(rho), ((1,), (1,)))
    xrecv[pl.ds(my_slot, 1)] = xsend[pl.ds(me, 1)]
    exchange(lambda t, slot: xsend.at[pl.ds(t, 1)], xrecv.at[pl.ds(my_slot, 1)], 1)

    freq = jnp.minimum(
        lax.broadcasted_iota(jnp.int32, (N, N), 0), N - lax.broadcasted_iota(jnp.int32, (N, N), 0)
    )
    freq_q = jnp.minimum(
        lax.broadcasted_iota(jnp.int32, (N, N), 1), N - lax.broadcasted_iota(jnp.int32, (N, N), 1)
    )
    freq_r = jnp.minimum(me, N - me)
    squared = freq * freq + freq_q * freq_q + freq_r * freq_r
    cell = N * spacing
    floored = jnp.maximum(squared, 1).astype(f32)
    coulomb = jnp.where(squared > 0, cell * cell / np.pi / floored, 0.0)

    arrived(xrecv, 1)
    joined = jnp.concatenate([xrecv[pl.ds(g * 32, 32)] for g in range(4)], axis=1)
    both = (wide[0], wide[1])
    second = product(halves(joined), both, ((1,), (0,)))
    stacked = jnp.concatenate([second[:, a * 128 : (a + 1) * 128] for a in range(4)], axis=0)
    spectrum = product((tab[2], tab[3]), halves(stacked), ((1,), (0,))) * coulomb
    back = product((tab[4], tab[5]), halves(spectrum), ((1,), (0,)))
    joined = jnp.concatenate([back[a * 32 : (a + 1) * 32] for a in range(4)], axis=1)
    planes = product(halves(joined), both, ((1,), (1,)))
    for g in range(4):
        vsend[pl.ds(g * 32, 32)] = planes[:, g * 128 : (g + 1) * 128]
    vrecv[pl.ds(me, 1)] = vsend[pl.ds(my_slot, 1)]
    exchange(lambda t, slot: vsend.at[pl.ds(slot, 1)], vrecv.at[pl.ds(me, 1)], 2)
    arrived(vrecv, 2)
    v_v[...] = product(halves(vrecv[...].T), basis, ((1,), (0,)))
    out_v = pltpu.make_async_copy(v_v, v_h, out_sem.at[1])
    out_v.start()

    for s in range(4):
        c_copy(s).wait_send()
        for step in plan[s]:
            for copy, _, _ in step:
                copy.wait_send()
    sent(grecv, 0)
    sent(xsend, 1)
    sent(vsend, 2)
    out_rho.wait()
    out_v.wait()


def local(orbitals, occupations, rho_in, hist_in, hist_res):
    anywhere = pl.BlockSpec(memory_space=pl.ANY)
    vmem, dma = pltpu.VMEM, pltpu.SemaphoreType.DMA
    square = (N, N)
    rho, v = pl.pallas_call(
        kernel,
        out_shape=[jax.ShapeDtypeStruct(square, f32)] * 2,
        in_specs=[anywhere, pl.BlockSpec(memory_space=pltpu.SMEM)] + [anywhere] * 4,
        out_specs=[anywhere] * 2,
        scratch_shapes=[
            vmem((8, N, 32, N), bf16), vmem(square, f32), vmem((HIST, N, N), f32),
            vmem((HIST, N, N), f32), vmem((6, N, N), bf16),
            vmem((4, 4, 2, 4, 32, N), f32), vmem((4, 4, 4, 32, N), f32),
            vmem((4, 2, 4, 32, N), f32), vmem((4, 4, 32, N), f32),
            vmem((4, 2, 32, N), f32), vmem((4, 32, N), f32),
            vmem((2, 512, 512), bf16), vmem((1, N), f32), vmem(square, f32),
            vmem(square, f32), vmem(square, f32), vmem(square, f32), vmem(square, f32),
            vmem(square, f32), vmem(square, f32),
            dma((CHUNKS,)), dma((4,)), dma((2,)), dma((4,)), dma((4,)),
            dma((24,)), dma((24,)), dma((3,)), dma((3,)),
        ],
        compiler_params=pltpu.CompilerParams(
            collective_id=0, has_side_effects=True, vmem_limit_bytes=40 * 2**20
        ),
    )(
        orbitals, occupations, rho_in.reshape(square), hist_in.reshape(HIST, N, N),
        hist_res.reshape(HIST, N, N), tables(),
    )
    return rho.reshape(rho_in.shape), v.reshape(rho_in.shape)


def solution(mesh):
    finer = Mesh(mesh.devices.reshape(4, 4, 2, 4), ("x", "y", "c", "z"))
    in_specs = (
        P(BAND, None, "z", None), P(BAND), P(BAND, "z", None),
        P(None, BAND, "z", None), P(None, BAND, "z", None),
    )
    out_specs = (P(BAND, "z", None), P(BAND, "z", None))
    return jax.shard_map(local, mesh=finer, in_specs=in_specs, out_specs=out_specs, check_vma=False)
```

```python
import functools

import jax
import jax.numpy as jnp
import numpy as np
from jax import lax
from jax.experimental import pallas as pl
from jax.experimental.pallas import tpu as pltpu
from jax.sharding import Mesh
from jax.sharding import PartitionSpec as P

LOGICAL = pl.DeviceIdType.LOGICAL
BAND = ("x", "y", "c")
N = 128
HIST = 7
beta_mix = 0.5
spacing = 0.2
f32 = jnp.float32
bf16 = jnp.bfloat16
STREAMS = (0, 2, 1, 3)
PIECES = [(h, s) for h in range(2) for s in STREAMS]
EARLY = 5
HIST_SENDS = (40, 60)


def tables():
    k = np.arange(N)
    angle = 2.0 * np.pi * ((k[:, None] * k[None, :]) % N) / N
    basis = (np.cos(angle) + np.sin(angle)) / np.sqrt(N)
    order = (4 * np.arange(32)[None, :] + np.arange(4)[:, None]).reshape(-1)
    parts = []
    for table in (basis, basis[:, order], basis[order, :]):
        high = table.astype(jnp.bfloat16)
        low = (table - high.astype(np.float64)).astype(jnp.bfloat16)
        parts += [high, low]
    return jnp.asarray(np.stack(parts))


def halves(value):
    high = value.astype(bf16)
    return high, (value - high.astype(f32)).astype(bf16)


def product(left, right, dims):
    dot = functools.partial(
        lax.dot_general, dimension_numbers=(dims, ((), ())), preferred_element_type=f32
    )
    return dot(left[0], right[0]) + (dot(left[0], right[1]) + dot(left[1], right[0]))


def partner_ids(x, y, c, z):
    plane = {(i, j): ((x + i) % 4) * 32 + ((y + j) % 4) * 8 for i in range(4) for j in range(4)}
    rest = {(i, j): ((c + i) % 2) * 4 + (z + j) % 4 for i in range(2) for j in range(4)}
    slot_plane = {(i, j): ((x + i) % 4) * 8 + ((y + j) % 4) * 2 for i in range(4) for j in range(4)}
    slot_rest = {(i, j): ((c + i) % 2) + ((z + j) % 4) * 32 for i in range(2) for j in range(4)}
    moves = [(a, b, d, e) for a in range(4) for b in range(4) for d in range(2) for e in range(4)][1:]

    def hops(m):
        return sum((0, 1, 2, 1)[m[i]] for i in (0, 1, 3))

    moves.sort(key=lambda m: -hops(m))
    return [
        (plane[m[:2]] + rest[m[2:]], slot_plane[m[:2]] + slot_rest[m[2:]], m) for m in moves
    ]


def regroup(rows):
    block = lax.broadcasted_iota(jnp.int32, (32, N), 1) // 32
    turned = {}
    for i in range(4):
        for j in range(4):
            shift = (i - j) % 4
            if (i, shift) not in turned:
                turned[i, shift] = rows[i] if shift == 0 else pltpu.roll(rows[i], 32 * shift, 1)
    out = []
    for j in range(4):
        value = turned[0, (0 - j) % 4]
        for i in range(1, 4):
            value = jnp.where(block == i, turned[i, (i - j) % 4], value)
        out.append(value)
    return out


def kernel(
    orb, occ, rin_h, hin_h, hres_h, tab_h, rho_h, v_h,
    orb_v, rin, hin, hres, tab, part, crecv, r1, r2, r3,
    hsend, hrecv, xsend, xrecv, vsend, vrecv,
    load_sem, in_sem, c_send, c_recv, rs_send, rs_recv, a_send, a_recv, z_sem,
):
    x, y, c, z = (lax.axis_index(a) for a in ("x", "y", "c", "z"))

    def place(px, py, pc, pz):
        return px * 32 + py * 8 + pc * 4 + pz

    me = place(x, y, c, z)
    my_slot = z * 32 + x * 8 + y * 2 + c
    others = partner_ids(x, y, c, z)

    barrier = pltpu.get_barrier_semaphore()
    near = [t for t, _, m in others if sum(v > 0 for v in m) == 1]
    for t in near:
        pl.semaphore_signal(barrier, inc=1, device_id=t, device_id_type=LOGICAL)

    def load(p):
        h, s = PIECES[p]
        return pltpu.make_async_copy(
            orb.at[:, :, s, pl.ds(h * 16, 16)], orb_v.at[p], load_sem.at[p]
        )

    for p in range(8):
        load(p).start()
    inputs = [(tab_h, tab), (hres_h, hres), (hin_h, hin), (rin_h, rin)]
    for i, (a, b) in enumerate(inputs):
        pltpu.make_async_copy(a, b, in_sem.at[i]).start()

    occupied = [occ[k] for k in range(8)]

    def density(p):
        h, s = PIECES[p]
        load(p).wait()

        @pl.loop(0, 4)
        def _(i):
            for row in range(8):
                total = None
                for k in range(8):
                    value = orb_v[p, k, i * 8 + row].astype(f32)
                    term = occupied[k] * (value * value)
                    total = term if total is None else total + term
                part[h, i, row // 2, row % 2, s] = total

    def c_copy(p):
        h, s = PIECES[p]
        return pltpu.make_async_remote_copy(
            src_ref=part.at[h, :, :, 1 - c, s], dst_ref=crecv.at[h, s],
            send_sem=c_send.at[p], recv_sem=c_recv.at[p],
            device_id=place(x, y, 1 - c, z), device_id_type=LOGICAL,
        )

    with jax.named_scope("density"):
        for p in range(EARLY):
            density(p)
    with jax.named_scope("barrier"):
        pl.semaphore_wait(barrier, len(near))
    with jax.named_scope("density_rest"):
        for p in range(EARLY):
            c_copy(p).start()
        for p in range(EARLY, 8):
            density(p)
            c_copy(p).start()

    flip = {
        "x": {1: x + 1 - 2 * (x % 2), 2: (x + 2) % 4, 3: 3 - x},
        "y": {1: y + 1 - 2 * (y % 2), 2: (y + 2) % 4, 3: 3 - y},
    }
    mine = {"x": x, "y": y}
    orders = {0: ("x", "y", 1), 1: ("x", "y", 3), 2: ("y", "x", 1), 3: ("y", "x", 3)}

    def dev(axis, e):
        if axis == "x":
            return place(flip["x"][e], y, c, z)
        return place(x, flip["y"][e], c, z)

    def steps(p):
        h, s = PIECES[p]
        first, second, e1 = orders[s]
        e2 = 4 - e1

        def remote(src, dst, sem, to):
            return pltpu.make_async_remote_copy(
                src_ref=src, dst_ref=dst, send_sem=rs_send.at[p * 6 + sem],
                recv_sem=rs_recv.at[p * 6 + sem], device_id=to, device_id_type=LOGICAL,
            )

        def rows_of(index):
            if first == "x":
                return part.at[h, index, :, c, s]
            return part.at[h, :, index, c, s]

        def block_of(index):
            if second == "x":
                return part.at[h, index, y, c, s]
            return part.at[h, x, index, c, s]

        one = [
            (remote(rows_of(flip[first][e1]), r1.at[h, s, 0], 0, dev(first, e1)),
             rows_of(mine[first]), r1.at[h, s, 0]),
            (remote(rows_of(flip[first][2]), r1.at[h, s, 1], 1, dev(first, e1)),
             rows_of(flip[first][e2]), r1.at[h, s, 1]),
        ]
        two = [
            (remote(rows_of(flip[first][e2]), r2.at[h, s], 2, dev(first, e2)),
             rows_of(mine[first]), r2.at[h, s]),
        ]
        three = [
            (remote(block_of(flip[second][e]), r3.at[h, s, e - 1], 2 + e, dev(second, e)),
             block_of(mine[second]), r3.at[h, s, e - 1])
            for e in (2, 1, 3)
        ]
        return [one, two, three]

    plan = [steps(p) for p in range(8)]

    def begin(p, step):
        for copy, _, _ in plan[p][step]:
            copy.start()

    def take(p, step):
        for copy, into, came in plan[p][step]:
            copy.wait_recv()
            into[...] = into[...] + came[...]

    with jax.named_scope("core_sum"):
        for p in range(8):
            h, s = PIECES[p]
            c_copy(p).wait_recv()
            own = part.at[h, :, :, c, s]
            own[...] = own[...] + crecv[h, s]
            begin(p, 0)
        for e in (1, 2, 3):
            pl.semaphore_signal(
                z_sem, inc=1, device_id=place(x, y, c, (z + e) % 4), device_id_type=LOGICAL
            )

    lane = lax.broadcasted_iota(jnp.int32, (8, N), 1)
    sub = lax.broadcasted_iota(jnp.int32, (8, N), 0)

    def fold(value):
        return jnp.sum(value.reshape(16, 8, N), axis=0)

    def products(field, amount):
        rows = jnp.zeros((8, N), f32)
        for j in range(amount):
            line = jnp.sum(fold(field * hres[j]), axis=0, keepdims=True)
            rows = jnp.where(sub == j, line, rows)
        return rows

    def placed(i, rows):
        total = jnp.sum(rows, axis=1, keepdims=True)
        spots = (lane == 8 * i + sub) | (lane == 8 * sub + i)
        return jnp.sum(jnp.where(spots & (sub <= i), total, 0.0), axis=0, keepdims=True)

    def every(start, count=N):
        return pl.ds(start, count, stride=8)

    with jax.named_scope("hist"):
        for i, (a, b) in enumerate(inputs):
            pltpu.make_async_copy(a, b, in_sem.at[i]).wait()
        basis = (tab[0], tab[1])
        for m in range(HIST):
            trial = hin[m] + beta_mix * hres[m]
            hsend[every(m), :] = product(basis, halves(trial), ((1,), (1,)))
        row = jnp.zeros((1, N), f32)
        for i in range(HIST):
            row = row + placed(i, products(hres[i], i + 1))
        hsend[every(7), :] = jnp.broadcast_to(row, (N, N))

    with jax.named_scope("step1"):
        for p in range(8):
            take(p, 0)
            if p == 0:
                pl.semaphore_wait(z_sem, 3)
            begin(p, 1)

    def exchange(pairs, source, target, sem):
        for t, slot, _ in pairs:
            pltpu.make_async_remote_copy(
                src_ref=source(t, slot), dst_ref=target,
                send_sem=a_send.at[sem], recv_sem=a_recv.at[sem],
                device_id=t, device_id_type=LOGICAL,
            ).start()

    def arrived(buffer, rows, sem):
        whole = buffer.at[pl.ds(0, 127 * rows)]
        pltpu.make_async_copy(whole, whole, a_recv.at[sem]).wait()

    def sent(buffer, rows, sem):
        whole = buffer.at[pl.ds(0, 127 * rows)]
        pltpu.make_async_copy(whole, whole, a_send.at[sem]).wait()

    def tile(index, rows):
        return pl.ds(pl.multiple_of(index * 8, 8), rows)

    def hist_exchange(pairs):
        exchange(pairs, lambda t, slot: hsend.at[tile(t, 8)], hrecv.at[tile(my_slot, 8)], 0)

    def unheard(o):
        return o[2][0] == 2 and o[2][1] == 2 and o[2][3] > 0

    hist_order = [o for o in others if not unheard(o)] + [o for o in others if unheard(o)]
    first, second = HIST_SENDS
    with jax.named_scope("step2a"):
        for p in range(4):
            take(p, 1)
            begin(p, 2)
    with jax.named_scope("hist_send1"):
        hist_exchange(hist_order[:first])
        hrecv[tile(my_slot, 8), :] = hsend[tile(me, 8), :]
    with jax.named_scope("step2b"):
        for p in range(4, 8):
            take(p, 1)
            begin(p, 2)
    with jax.named_scope("hist_send2"):
        hist_exchange(hist_order[first : first + second])
    with jax.named_scope("step3"):
        for p in range(8):
            take(p, 2)

    with jax.named_scope("new"):
        blocks = [part[h, x, y, c, s] for s in range(4) for h in range(2)]
        new = jnp.concatenate(blocks, axis=0) - rin[...]
        xsend[every(0), :] = product(basis, halves(rin[...] + beta_mix * new), ((1,), (1,)))
        rows = products(new, HIST)
        rows = jnp.where(sub == 7, jnp.sum(fold(new * new), axis=0, keepdims=True), rows)
        row = placed(7, rows)
        xsend[every(1), :] = jnp.broadcast_to(row, (N, N))
    with jax.named_scope("x_send"):
        exchange(others, lambda t, slot: xsend.at[tile(t, 2)], xrecv.at[tile(my_slot, 2)], 1)
        xrecv[tile(my_slot, 2), :] = xsend[tile(me, 2), :]
    with jax.named_scope("hist_send3"):
        hist_exchange(hist_order[first + second :])

    with jax.named_scope("coulomb"):
        p_index = lax.broadcasted_iota(jnp.int32, (N, N), 0)
        q_index = lax.broadcasted_iota(jnp.int32, (N, N), 1)
        freq_p = jnp.minimum(p_index, N - p_index)
        freq_q = jnp.minimum(q_index, N - q_index)
        freq_r = jnp.minimum(me, N - me)
        squared = freq_p * freq_p + freq_q * freq_q + freq_r * freq_r
        cell = N * spacing
        floored = jnp.maximum(squared, 1).astype(f32)
        coulomb = jnp.where(squared > 0, cell * cell / np.pi / floored, 0.0)

    with jax.named_scope("hist_wait"):
        arrived(hrecv, 8, 0)
    with jax.named_scope("x_wait"):
        arrived(xrecv, 2, 1)

    with jax.named_scope("solve"):
        flat = jnp.sum(xrecv[every(1), :], axis=0, keepdims=True)
        flat = (flat + jnp.sum(hrecv[every(7), :], axis=0, keepdims=True)) * (1.0 / (N * N * N))
        matrix = jnp.zeros((8, N), f32)
        for i in range(8):
            shifted = flat if i == 0 else pltpu.roll(flat, N - 8 * i, 1)
            matrix = jnp.where(sub == i, shifted, matrix)
        matrix = jnp.where(lane < 8, matrix, jnp.where(lane == 8, 1.0, 0.0))
        for k in range(8):
            pivot_row = matrix[k : k + 1, :]
            column = jnp.sum(jnp.where(lane == k, matrix, 0.0), axis=1, keepdims=True)
            pivot = column[k : k + 1, :]
            matrix = jnp.where(sub == k, matrix, matrix - (column / pivot) * pivot_row)
        diagonal = jnp.sum(jnp.where(lane == sub, matrix, 0.0), axis=1, keepdims=True)
        right = jnp.sum(jnp.where(lane == 8, matrix, 0.0), axis=1, keepdims=True)
        solved = right / diagonal
        weights = solved / jnp.sum(solved, axis=0, keepdims=True)

    with jax.named_scope("planes"):
        plane = weights[7:8, :] * xrecv[every(0), :]
        for m in range(HIST):
            plane = plane + weights[m : m + 1, :] * hrecv[every(m), :]
        grouped = jnp.concatenate(regroup([plane[g * 32 : (g + 1) * 32] for g in range(4)]), axis=0)
        second = product(halves(grouped), basis, ((1,), (0,)))
        spectrum = product((tab[2], tab[3]), halves(second), ((1,), (0,))) * coulomb
        back = product((tab[4], tab[5]), halves(spectrum), ((1,), (0,)))
        back = product(halves(back), basis, ((1,), (0,)))
        back = regroup([back[a * 32 : (a + 1) * 32] for a in range(4)])
        vsend[...] = jnp.concatenate(back, axis=0)
    with jax.named_scope("v_send"):
        exchange(others, lambda t, slot: vsend.at[pl.ds(slot, 1)], vrecv.at[pl.ds(me, 1)], 2)
        vrecv[pl.ds(me, 1)] = vsend[pl.ds(my_slot, 1)]

    with jax.named_scope("mix"):
        rho = weights[7:8, :] * (rin[...] + beta_mix * new)
        for m in range(HIST):
            rho = rho + weights[m : m + 1, :] * (hin[m] + beta_mix * hres[m])
        rho_h[...] = rho
        for p in range(8):
            c_copy(p).wait_send()
            for step in plan[p]:
                for copy, _, _ in step:
                    copy.wait_send()
        sent(hsend, 8, 0)
        sent(xsend, 2, 1)

    with jax.named_scope("v_wait"):
        arrived(vrecv, 1, 2)
    with jax.named_scope("last"):
        v_h[...] = product(halves(vrecv[...].T), basis, ((1,), (0,)))
    sent(vsend, 1, 2)


def local(orbitals, occupations, rho_in, hist_in, hist_res):
    anywhere = pl.BlockSpec(memory_space=pl.ANY)
    vmem, dma = pltpu.VMEM, pltpu.SemaphoreType.DMA
    square = (N, N)
    rho, v = pl.pallas_call(
        kernel,
        out_shape=[jax.ShapeDtypeStruct(square, f32)] * 2,
        in_specs=[anywhere, pl.BlockSpec(memory_space=pltpu.SMEM)] + [anywhere] * 4,
        out_specs=[pl.BlockSpec(memory_space=pltpu.VMEM)] * 2,
        scratch_shapes=[
            vmem((8, 8, 32, 16, N), bf16), vmem(square, f32), vmem((HIST, N, N), f32),
            vmem((HIST, N, N), f32), vmem((6, N, N), bf16),
            vmem((2, 4, 4, 2, 4, 16, N), f32), vmem((2, 4, 4, 4, 16, N), f32),
            vmem((2, 4, 2, 4, 16, N), f32), vmem((2, 4, 4, 16, N), f32),
            vmem((2, 4, 3, 16, N), f32),
            vmem((8 * N, N), f32), vmem((8 * N, N), f32), vmem((8 * N, N), f32),
            vmem((8 * N, N), f32), vmem(square, f32), vmem(square, f32),
            dma((8,)), dma((4,)), dma((8,)), dma((8,)),
            dma((48,)), dma((48,)), dma((3,)), dma((3,)), pltpu.SemaphoreType.REGULAR,
        ],
        compiler_params=pltpu.CompilerParams(
            collective_id=0, has_side_effects=True, vmem_limit_bytes=67043328
        ),
    )(
        orbitals.reshape(8, 32, 4, 32, N), occupations, rho_in.reshape(square),
        hist_in.reshape(HIST, N, N), hist_res.reshape(HIST, N, N), tables(),
    )
    return rho.reshape(rho_in.shape), v.reshape(rho_in.shape)


def solution(mesh):
    finer = Mesh(mesh.devices.reshape(4, 4, 2, 4), ("x", "y", "c", "z"))
    in_specs = (
        P(BAND, None, "z", None), P(BAND), P(BAND, "z", None),
        P(None, BAND, "z", None), P(None, BAND, "z", None),
    )
    out_specs = (P(BAND, "z", None), P(BAND, "z", None))
    return jax.shard_map(local, mesh=finer, in_specs=in_specs, out_specs=out_specs, check_vma=False)
```

```python
import functools

import jax
import jax.numpy as jnp
import numpy as np
from jax import lax
from jax.experimental import pallas as pl
from jax.experimental.pallas import tpu as pltpu
from jax.sharding import Mesh
from jax.sharding import PartitionSpec as P

LOGICAL = pl.DeviceIdType.LOGICAL
BAND = ("x", "y", "c")
N = 128
HIST = 7
beta_mix = 0.5
spacing = 0.2
f32 = jnp.float32
bf16 = jnp.bfloat16
STREAMS = (0, 2, 1, 3)
PARTS = 4
ROWS = 32 // PARTS
PIECES = [(h, s) for h in range(2) for s in STREAMS]
SENDS = [(h, s) for h in range(PARTS) for s in STREAMS]
EARLY = 1
LAG = 4
STAGES = (0, 0, 0, 119)
REST_AT = 2


def tables():
    k = np.arange(N)
    angle = 2.0 * np.pi * ((k[:, None] * k[None, :]) % N) / N
    basis = (np.cos(angle) + np.sin(angle)) / np.sqrt(N)
    order = (4 * np.arange(32)[None, :] + np.arange(4)[:, None]).reshape(-1)
    parts = []
    for table in (basis, basis[:, order], basis[order, :]):
        high = table.astype(jnp.bfloat16)
        low = (table - high.astype(np.float64)).astype(jnp.bfloat16)
        parts += [high, low]
    return jnp.asarray(np.stack(parts))


def halves(value):
    high = value.astype(bf16)
    return high, (value - high.astype(f32)).astype(bf16)


def product(left, right, dims):
    dot = functools.partial(
        lax.dot_general, dimension_numbers=(dims, ((), ())), preferred_element_type=f32
    )
    return dot(left[0], right[0]) + (dot(left[0], right[1]) + dot(left[1], right[0]))


def partner_ids(x, y, c, z):
    plane = {(i, j): ((x + i) % 4) * 32 + ((y + j) % 4) * 8 for i in range(4) for j in range(4)}
    rest = {(i, j): ((c + i) % 2) * 4 + (z + j) % 4 for i in range(2) for j in range(4)}
    slot_plane = {(i, j): ((x + i) % 4) * 8 + ((y + j) % 4) * 2 for i in range(4) for j in range(4)}
    slot_rest = {(i, j): ((c + i) % 2) + ((z + j) % 4) * 32 for i in range(2) for j in range(4)}
    moves = [(a, b, d, e) for a in range(4) for b in range(4) for d in range(2) for e in range(4)][1:]

    def hops(m):
        return sum((0, 1, 2, 1)[m[i]] for i in (0, 1, 3))

    moves.sort(key=lambda m: -hops(m))
    return [
        (plane[m[:2]] + rest[m[2:]], slot_plane[m[:2]] + slot_rest[m[2:]], m) for m in moves
    ]


def regroup(rows):
    block = lax.broadcasted_iota(jnp.int32, (32, N), 1) // 32
    turned = {}
    for i in range(4):
        for j in range(4):
            shift = (i - j) % 4
            if (i, shift) not in turned:
                turned[i, shift] = rows[i] if shift == 0 else pltpu.roll(rows[i], 32 * shift, 1)
    out = []
    for j in range(4):
        value = turned[0, (0 - j) % 4]
        for i in range(1, 4):
            value = jnp.where(block == i, turned[i, (i - j) % 4], value)
        out.append(value)
    return out


def kernel(
    orb, occ_h, rin_h, hin_h, hres_h, tab_h, rho_h, v_h,
    orb_v, occ, rin, hin, hres, tab, part, crecv, r1, r2,
    hsend, hrecv, xsend, xrecv, vsend, vrecv,
    load_sem, in_sem, c_recv, r_send, rs_recv, a_send, a_recv, z_sem,
):
    x, y, c, z = (lax.axis_index(a) for a in ("x", "y", "c", "z"))

    def place(px, py, pc, pz):
        return px * 32 + py * 8 + pc * 4 + pz

    me = place(x, y, c, z)
    my_slot = z * 32 + x * 8 + y * 2 + c
    def load(p):
        h, s = PIECES[p]
        return pltpu.make_async_copy(
            orb.at[:, :, s, pl.ds(h * 16, 16)], orb_v.at[p], load_sem.at[p]
        )

    occ_copy = pltpu.make_async_copy(occ_h, occ, in_sem.at[4])
    occ_copy.start()
    load(0).start()
    barrier = pltpu.get_barrier_semaphore()
    near = [place(x, y, 1 - c, z)]
    for e in (2, 1, 3):
        near += [
            place((x + e) % 4, y, c, z), place(x, (y + e) % 4, c, z), place(x, y, c, (z + e) % 4)
        ]
    for t in near:
        pl.semaphore_signal(barrier, inc=1, device_id=t, device_id_type=LOGICAL)
    for p in range(1, 8):
        load(p).start()
    inputs = [(tab_h, tab), (hres_h, hres), (hin_h, hin), (rin_h, rin)]
    for i, (a, b) in enumerate(inputs):
        pltpu.make_async_copy(a, b, in_sem.at[i]).start()

    occ_copy.wait()
    occupied = [occ[k] for k in range(8)]

    def density(p):
        h, s = PIECES[p]
        load(p).wait()

        @pl.loop(0, 4)
        def _(i):
            for row in range(8):
                total = None
                for k in range(8):
                    value = orb_v[p, k, i * 8 + row].astype(f32)
                    term = occupied[k] * (value * value)
                    total = term if total is None else total + term
                for k in range(PARTS // 2):
                    part[h * (PARTS // 2) + k, i, row // 2, row % 2, s] = total[
                        k * ROWS : (k + 1) * ROWS
                    ]

    def c_copy(p):
        h, s = SENDS[p]
        return pltpu.make_async_remote_copy(
            src_ref=part.at[h, :, :, 1 - c, s], dst_ref=crecv.at[h, s],
            send_sem=r_send.at[0], recv_sem=c_recv.at[PIECES.index((h // (PARTS // 2), s))],
            device_id=place(x, y, 1 - c, z), device_id_type=LOGICAL,
        )

    def c_begin(p):
        h, s = PIECES[p]
        for k in range(PARTS // 2):
            c_copy(SENDS.index((h * (PARTS // 2) + k, s))).start()

    flip = {
        "x": {1: x + 1 - 2 * (x % 2), 2: (x + 2) % 4, 3: 3 - x},
        "y": {1: y + 1 - 2 * (y % 2), 2: (y + 2) % 4, 3: 3 - y},
    }
    mine = {"x": x, "y": y}
    orders = {0: ("x", "y", 1), 1: ("x", "y", 3), 2: ("y", "x", 1), 3: ("y", "x", 3)}

    def dev(axis, e):
        if axis == "x":
            return place(flip["x"][e], y, c, z)
        return place(x, flip["y"][e], c, z)

    def steps(p):
        h, s = SENDS[p]
        first, second, e1 = orders[s]
        e2 = 4 - e1

        def remote(src, dst, sem, to):
            return pltpu.make_async_remote_copy(
                src_ref=src, dst_ref=dst, send_sem=r_send.at[1 + sem],
                recv_sem=rs_recv.at[PARTS * sem + h], device_id=to, device_id_type=LOGICAL,
            )

        def rows_of(index):
            if first == "x":
                return part.at[h, index, :, c, s]
            return part.at[h, :, index, c, s]

        def spot(i, j):
            return (i, j) if first == "x" else (j, i)

        one = [
            (remote(rows_of(flip[first][e1]), r1.at[h, s, 0], 0, dev(first, e1)),
             rows_of(mine[first]), r1.at[h, s, 0]),
            (remote(rows_of(flip[first][2]), r1.at[h, s, 1], 0, dev(first, e1)),
             rows_of(flip[first][e2]), r1.at[h, s, 1]),
        ]
        two = []
        moves = [(e2, 2), (e2, 1), (e2, 3), (0, 2), (e2, 0), (0, 1), (0, 3)]
        for n, (i, j) in enumerate(moves):
            to_x, to_y = spot(
                flip[first][i] if i else mine[first], flip[second][j] if j else mine[second]
            )
            two.append(remote(
                part.at[h, to_x, to_y, c, s], r2.at[h, s, n], 1, place(to_x, to_y, c, z)
            ))
        return one, two

    plan = [steps(p) for p in range(4 * PARTS)]

    def bytes_of(ref, sem):
        pltpu.make_async_copy(ref, ref, sem).wait()

    def core_sum(p):
        half, s = PIECES[p]
        inner = PARTS // 2
        bytes_of(crecv.at[pl.ds(half * inner, inner), s], c_recv.at[p])
        for h in range(half * inner, (half + 1) * inner):
            own = part.at[h, :, :, c, s]
            own[...] = own[...] + crecv[h, s]
            for copy, _, _ in plan[SENDS.index((h, s))][0]:
                copy.start()

    others = partner_ids(x, y, c, z)

    for p in range(8):
        with jax.named_scope(f"density_{p}"):
            density(p)
        if p == EARLY - 1:
            with jax.named_scope("barrier"):
                pl.semaphore_wait(barrier, len(near))
            for q in range(EARLY):
                c_begin(q)
        elif p >= EARLY:
            c_begin(p)
        if p - LAG >= 0 and p >= EARLY:
            with jax.named_scope(f"core_{p}"):
                core_sum(p - LAG)
    with jax.named_scope("core_rest"):
        for p in range(8 - LAG, 8):
            core_sum(p)

    lane = lax.broadcasted_iota(jnp.int32, (8, N), 1)
    sub = lax.broadcasted_iota(jnp.int32, (8, N), 0)

    def fold(value):
        return jnp.sum(value.reshape(16, 8, N), axis=0)

    def products(field, amount):
        rows = jnp.zeros((8, N), f32)
        for j in range(amount):
            line = jnp.sum(fold(field * hres[j]), axis=0, keepdims=True)
            rows = jnp.where(sub == j, line, rows)
        return rows

    def placed(i, rows):
        total = jnp.sum(rows, axis=1, keepdims=True)
        spots = (lane == 8 * i + sub) | (lane == 8 * sub + i)
        return jnp.sum(jnp.where(spots & (sub <= i), total, 0.0), axis=0, keepdims=True)

    def every(start, count=N):
        return pl.ds(start, count, stride=8)

    with jax.named_scope("hist"):
        for i, (a, b) in enumerate(inputs):
            pltpu.make_async_copy(a, b, in_sem.at[i]).wait()
        basis = (tab[0], tab[1])
        for m in range(HIST):
            trial = hin[m] + beta_mix * hres[m]
            hsend[every(m), :] = product(basis, halves(trial - 1.0), ((1,), (1,)))
        row = jnp.zeros((1, N), f32)
        for i in range(HIST):
            row = row + placed(i, products(hres[i], i + 1))
        early_row = row

    def exchange(pairs, source, target, sem):
        for t, slot, _ in pairs:
            pltpu.make_async_remote_copy(
                src_ref=source(t, slot), dst_ref=target,
                send_sem=a_send.at[sem], recv_sem=a_recv.at[sem],
                device_id=t, device_id_type=LOGICAL,
            ).start()

    def arrived(buffer, rows, sem):
        whole = buffer.at[pl.ds(0, 127 * rows)]
        pltpu.make_async_copy(whole, whole, a_recv.at[sem]).wait()

    def sent(buffer, rows, sem):
        whole = buffer.at[pl.ds(0, 127 * rows)]
        pltpu.make_async_copy(whole, whole, a_send.at[sem]).wait()

    def tile(index, rows):
        return pl.ds(pl.multiple_of(index * 8, 8), rows)

    def hist_exchange(pairs):
        exchange(pairs, lambda t, slot: hsend.at[tile(t, 7)], hrecv.at[tile(my_slot, 7)], 0)

    def unheard(o):
        return o[2][0] == 2 and o[2][1] == 2

    hist_order = sorted(others, key=lambda o: (unheard(o), o[2][3] > 0))
    ends = np.cumsum((0,) + STAGES)
    def hist_stage(h):
        if h == 0:
            hrecv[tile(my_slot, 7), :] = hsend[tile(me, 7), :]
        with jax.named_scope(f"hist_send{h}"):
            if ends[h] <= 29 < ends[h + 1]:
                pl.semaphore_wait(z_sem, 3)
            hist_exchange(hist_order[ends[h] : ends[h + 1]])

    for h in range(PARTS):
        with jax.named_scope(f"step1_{h}"):
            bytes_of(r1.at[h], rs_recv.at[h])
            for p in range(4 * h, 4 * h + 4):
                for _, into, came in plan[p][0]:
                    into[...] = into[...] + came[...]
            if h == 0:
                for e in (1, 2, 3):
                    pl.semaphore_signal(
                        z_sem, inc=1, device_id=place(x, y, c, (z + e) % 4), device_id_type=LOGICAL
                    )
            for p in range(4 * h, 4 * h + 4):
                for copy in plan[p][1]:
                    copy.start()
        hist_stage(h)

    for h in range(PARTS):
        with jax.named_scope(f"step2_{h}"):
            bytes_of(r2.at[h], rs_recv.at[PARTS + h])
            if h == REST_AT:
                hist_exchange(hist_order[ends[-1] :])

    with jax.named_scope("new"):
        blocks = []
        for s in range(4):
            for h in range(PARTS):
                total = part[h, x, y, c, s]
                for n in range(7):
                    total = total + r2[h, s, n]
                blocks.append(total)
        new = jnp.concatenate(blocks, axis=0) - rin[...]
        xsend[every(0), :] = product(basis, halves((rin[...] - 1.0) + beta_mix * new), ((1,), (1,)))
        rows = products(new, HIST)
        rows = jnp.where(sub == 7, jnp.sum(fold(new * new), axis=0, keepdims=True), rows)
        row = early_row + placed(7, rows)
        xsend[every(1), :] = jnp.broadcast_to(row, (N, N))
    with jax.named_scope("x_send"):
        exchange(others, lambda t, slot: xsend.at[tile(t, 2)], xrecv.at[tile(my_slot, 2)], 1)
        xrecv[tile(my_slot, 2), :] = xsend[tile(me, 2), :]
    with jax.named_scope("coulomb"):
        p_index = lax.broadcasted_iota(jnp.int32, (N, N), 0)
        q_index = lax.broadcasted_iota(jnp.int32, (N, N), 1)
        freq_p = jnp.minimum(p_index, N - p_index)
        freq_q = jnp.minimum(q_index, N - q_index)
        freq_r = jnp.minimum(me, N - me)
        squared = freq_p * freq_p + freq_q * freq_q + freq_r * freq_r
        cell = N * spacing
        floored = jnp.maximum(squared, 1).astype(f32)
        coulomb = jnp.where(squared > 0, cell * cell / np.pi / floored, 0.0)

    with jax.named_scope("x_wait"):
        arrived(xrecv, 2, 1)
    with jax.named_scope("hist_wait"):
        arrived(hrecv, 7, 0)

    with jax.named_scope("solve"):
        flat = jnp.sum(xrecv[every(1), :], axis=0, keepdims=True)
        flat = flat * (1.0 / (N * N * N))
        entry = {
            (i, j): jnp.broadcast_to(flat[:, 8 * i + j : 8 * i + j + 1], (8, N))
            for i in range(8) for j in range(i + 1)
        }
        right = [jnp.ones((8, N), f32) for _ in range(8)]
        inverse = []
        for k in range(8):
            inverse.append(1.0 / entry[k, k])
            ratio = {i: entry[i, k] * inverse[k] for i in range(k + 1, 8)}
            for i in range(k + 1, 8):
                right[i] = right[i] - ratio[i] * right[k]
                for j in range(k + 1, i + 1):
                    entry[i, j] = entry[i, j] - ratio[i] * entry[j, k]
            for i in range(k + 1, 8):
                entry[i, k] = ratio[i]
        solved = [right[k] * inverse[k] for k in range(8)]
        for k in range(7, -1, -1):
            for i in range(k):
                solved[i] = solved[i] - entry[k, i] * solved[k]
        total = functools.reduce(lambda a, b: a + b, solved)
        weights = [(value / total)[:1] for value in solved]

    with jax.named_scope("planes"):
        plane = weights[7] * xrecv[every(0), :]
        for m in range(HIST):
            plane = plane + weights[m] * hrecv[every(m), :]
        grouped = jnp.concatenate(regroup([plane[g * 32 : (g + 1) * 32] for g in range(4)]), axis=0)
        second = product(halves(grouped), basis, ((1,), (0,)))
        spectrum = product((tab[2], tab[3]), halves(second), ((1,), (0,))) * coulomb
        back = product((tab[4], tab[5]), halves(spectrum), ((1,), (0,)))
        back = product(halves(back), basis, ((1,), (0,)))
        back = regroup([back[a * 32 : (a + 1) * 32] for a in range(4)])
        vsend[...] = jnp.concatenate(back, axis=0)
    with jax.named_scope("v_send"):
        exchange(others, lambda t, slot: vsend.at[pl.ds(slot, 1)], vrecv.at[pl.ds(me, 1)], 2)
        vrecv[pl.ds(me, 1)] = vsend[pl.ds(my_slot, 1)]

    with jax.named_scope("mix"):
        rho = weights[7] * (rin[...] + beta_mix * new)
        for m in range(HIST):
            rho = rho + weights[m] * (hin[m] + beta_mix * hres[m])
        rho_h[...] = rho
    with jax.named_scope("drain"):
        bytes_of(crecv, r_send.at[0])
        bytes_of(r1, r_send.at[1])
        bytes_of(r2, r_send.at[2])
        sent(hsend, 7, 0)
        sent(xsend, 2, 1)

    with jax.named_scope("v_wait"):
        arrived(vrecv, 1, 2)
    with jax.named_scope("last"):
        v_h[...] = product(halves(vrecv[...].T), basis, ((1,), (0,)))
    sent(vsend, 1, 2)


def local(orbitals, occupations, rho_in, hist_in, hist_res):
    anywhere = pl.BlockSpec(memory_space=pl.ANY)
    vmem, dma = pltpu.VMEM, pltpu.SemaphoreType.DMA
    square = (N, N)
    rho, v = pl.pallas_call(
        kernel,
        out_shape=[pltpu.VMEM(square, f32)] * 2,
        in_specs=[anywhere] * 6,
        out_specs=[pl.BlockSpec(memory_space=pltpu.VMEM)] * 2,
        scratch_shapes=[
            vmem((8, 8, 32, 16, N), bf16), pltpu.SMEM((8,), f32), vmem(square, f32), vmem((HIST, N, N), f32),
            vmem((HIST, N, N), f32), vmem((6, N, N), bf16),
            vmem((PARTS, 4, 4, 2, 4, ROWS, N), f32), vmem((PARTS, 4, 4, 4, ROWS, N), f32),
            vmem((PARTS, 4, 2, 4, ROWS, N), f32), vmem((PARTS, 4, 7, ROWS, N), f32),
            vmem((8 * N, N), f32), vmem((8 * N, N), f32), vmem((8 * N, N), f32),
            vmem((8 * N, N), f32), vmem(square, f32), vmem(square, f32),
            dma((8,)), dma((5,)), dma((8,)), dma((3,)), dma((2 * PARTS,)), dma((3,)), dma((3,)), pltpu.SemaphoreType.REGULAR,
        ],
        compiler_params=pltpu.CompilerParams(
            collective_id=0, has_side_effects=True, vmem_limit_bytes=67043328 - 163840
        ),
    )(
        orbitals.reshape(8, 32, 4, 32, N), occupations, rho_in.reshape(square),
        hist_in.reshape(HIST, N, N), hist_res.reshape(HIST, N, N), tables(),
    )
    return rho.reshape(rho_in.shape), v.reshape(rho_in.shape)


def solution(mesh):
    finer = Mesh(mesh.devices.reshape(4, 4, 2, 4), ("x", "y", "c", "z"))
    in_specs = (
        P(BAND, None, "z", None), P(BAND), P(BAND, "z", None),
        P(None, BAND, "z", None), P(None, BAND, "z", None),
    )
    out_specs = (P(BAND, "z", None), P(BAND, "z", None))
    return jax.shard_map(local, mesh=finer, in_specs=in_specs, out_specs=out_specs, check_vma=False)
```

```python
import functools

import jax
import jax.numpy as jnp
import numpy as np
from jax import lax
from jax.experimental import pallas as pl
from jax.experimental.pallas import tpu as pltpu
from jax.sharding import Mesh
from jax.sharding import PartitionSpec as P

LOGICAL = pl.DeviceIdType.LOGICAL
BAND = ("x", "y", "c")
N = 128
HIST = 7
beta_mix = 0.5
spacing = 0.2
f32 = jnp.float32
bf16 = jnp.bfloat16
STREAMS = (0, 2, 1, 3)
PARTS = 4
ROWS = 32 // PARTS
PIECES = [(h, s) for h in range(2) for s in STREAMS]
SENDS = [(h, s) for h in range(PARTS) for s in STREAMS]
EARLY = 1
LAG = 5
STAGES = (0, 0, 0, 119)
REST_AT = 2


def tables():
    k = np.arange(N)
    angle = 2.0 * np.pi * ((k[:, None] * k[None, :]) % N) / N
    basis = (np.cos(angle) + np.sin(angle)) / np.sqrt(N)
    high = basis.astype(jnp.bfloat16)
    low = (basis - high.astype(np.float64)).astype(jnp.bfloat16).astype(np.float64)
    leak = (high.astype(np.float64) + low)[1:].sum(axis=1)
    low[1:, 0] -= leak
    low[0, 1:] -= leak
    low = low.astype(jnp.bfloat16)
    order = (4 * np.arange(32)[None, :] + np.arange(4)[:, None]).reshape(-1)
    parts = []
    for index in ((slice(None), slice(None)), (slice(None), order), (order, slice(None))):
        parts += [high[index], low[index]]
    return jnp.asarray(np.stack(parts))


def halves(value):
    high = value.astype(bf16)
    return high, (value - high.astype(f32)).astype(bf16)


def product(left, right, dims):
    (k_left,), (k_right,) = dims
    deep = jnp.concatenate(left, axis=k_left)
    tall = jnp.concatenate([right[0], right[0]], axis=k_right)
    dot = functools.partial(
        lax.dot_general, dimension_numbers=(dims, ((), ())), preferred_element_type=f32
    )
    return dot(deep, tall) + dot(left[0], right[1])


def partner_ids(x, y, c, z):
    plane = {(i, j): ((x + i) % 4) * 32 + ((y + j) % 4) * 8 for i in range(4) for j in range(4)}
    rest = {(i, j): ((c + i) % 2) * 4 + (z + j) % 4 for i in range(2) for j in range(4)}
    slot_plane = {(i, j): ((x + i) % 4) * 8 + ((y + j) % 4) * 2 for i in range(4) for j in range(4)}
    slot_rest = {(i, j): ((c + i) % 2) + ((z + j) % 4) * 32 for i in range(2) for j in range(4)}
    moves = [(a, b, d, e) for a in range(4) for b in range(4) for d in range(2) for e in range(4)][1:]

    def hops(m):
        return sum((0, 1, 2, 1)[m[i]] for i in (0, 1, 3))

    moves.sort(key=lambda m: -hops(m))
    return [
        (plane[m[:2]] + rest[m[2:]], slot_plane[m[:2]] + slot_rest[m[2:]], m) for m in moves
    ]


def regroup(rows):
    block = lax.broadcasted_iota(jnp.int32, (32, N), 1) // 32
    turned = {}
    for i in range(4):
        for j in range(4):
            shift = (i - j) % 4
            if (i, shift) not in turned:
                turned[i, shift] = rows[i] if shift == 0 else pltpu.roll(rows[i], 32 * shift, 1)
    out = []
    for j in range(4):
        value = turned[0, (0 - j) % 4]
        for i in range(1, 4):
            value = jnp.where(block == i, turned[i, (i - j) % 4], value)
        out.append(value)
    return out


def kernel(
    orb, occ_h, rin_h, hin_h, hres_h, tab_h, rho_h, v_h,
    orb_v, occ, rin, hin, hres, tab, part, crecv, r1, r2,
    hsend, hrecv, xsend, xrecv, vsend, vrecv,
    load_sem, in_sem, c_recv, r_send, rs_recv, a_send, a_recv, z_sem,
):
    x, y, c, z = (lax.axis_index(a) for a in ("x", "y", "c", "z"))

    def place(px, py, pc, pz):
        return px * 32 + py * 8 + pc * 4 + pz

    me = place(x, y, c, z)
    my_slot = z * 32 + x * 8 + y * 2 + c
    def load(p):
        h, s = PIECES[p]
        return pltpu.make_async_copy(
            orb.at[:, :, s, pl.ds(h * 16, 16)], orb_v.at[p], load_sem.at[p]
        )

    occ_copy = pltpu.make_async_copy(occ_h, occ, in_sem.at[4])
    occ_copy.start()
    load(0).start()
    barrier = pltpu.get_barrier_semaphore()
    near = [place(x, y, 1 - c, z)]
    for e in (2, 1, 3):
        near += [
            place((x + e) % 4, y, c, z), place(x, (y + e) % 4, c, z), place(x, y, c, (z + e) % 4)
        ]
    for t in near:
        pl.semaphore_signal(barrier, inc=1, device_id=t, device_id_type=LOGICAL)
    for p in range(1, 8):
        load(p).start()
    inputs = [(tab_h, tab), (hres_h, hres), (hin_h, hin), (rin_h, rin)]
    for i, (a, b) in enumerate(inputs):
        pltpu.make_async_copy(a, b, in_sem.at[i]).start()

    occ_copy.wait()
    occupied = [occ[k] for k in range(8)]

    def density(p):
        h, s = PIECES[p]
        load(p).wait()

        @pl.loop(0, 4)
        def _(i):
            for row in range(8):
                total = None
                for k in range(8):
                    value = orb_v[p, k, i * 8 + row].astype(f32)
                    term = occupied[k] * (value * value)
                    total = term if total is None else total + term
                for k in range(PARTS // 2):
                    part[h * (PARTS // 2) + k, i, row // 2, row % 2, s] = total[
                        k * ROWS : (k + 1) * ROWS
                    ]

    def c_copy(p):
        h, s = SENDS[p]
        return pltpu.make_async_remote_copy(
            src_ref=part.at[h, :, :, 1 - c, s], dst_ref=crecv.at[h, s],
            send_sem=r_send.at[0], recv_sem=c_recv.at[PIECES.index((h // (PARTS // 2), s))],
            device_id=place(x, y, 1 - c, z), device_id_type=LOGICAL,
        )

    def c_begin(p):
        h, s = PIECES[p]
        for k in range(PARTS // 2):
            c_copy(SENDS.index((h * (PARTS // 2) + k, s))).start()

    flip = {
        "x": {1: x + 1 - 2 * (x % 2), 2: (x + 2) % 4, 3: 3 - x},
        "y": {1: y + 1 - 2 * (y % 2), 2: (y + 2) % 4, 3: 3 - y},
    }
    mine = {"x": x, "y": y}
    orders = {0: ("x", "y", 1), 1: ("x", "y", 3), 2: ("y", "x", 1), 3: ("y", "x", 3)}

    def dev(axis, e):
        if axis == "x":
            return place(flip["x"][e], y, c, z)
        return place(x, flip["y"][e], c, z)

    def steps(p):
        h, s = SENDS[p]
        first, second, e1 = orders[s]
        e2 = 4 - e1

        def remote(src, dst, sem, to):
            return pltpu.make_async_remote_copy(
                src_ref=src, dst_ref=dst, send_sem=r_send.at[1 + sem],
                recv_sem=rs_recv.at[PARTS * sem + h], device_id=to, device_id_type=LOGICAL,
            )

        def rows_of(index):
            if first == "x":
                return part.at[h, index, :, c, s]
            return part.at[h, :, index, c, s]

        def spot(i, j):
            return (i, j) if first == "x" else (j, i)

        one = [
            (remote(rows_of(flip[first][e1]), r1.at[h, s, 0], 0, dev(first, e1)),
             rows_of(mine[first]), r1.at[h, s, 0]),
            (remote(rows_of(flip[first][2]), r1.at[h, s, 1], 0, dev(first, e1)),
             rows_of(flip[first][e2]), r1.at[h, s, 1]),
        ]
        two = []
        moves = [(e2, 2), (e2, 1), (e2, 3), (0, 2), (e2, 0), (0, 1), (0, 3)]
        for n, (i, j) in enumerate(moves):
            to_x, to_y = spot(
                flip[first][i] if i else mine[first], flip[second][j] if j else mine[second]
            )
            two.append(remote(
                part.at[h, to_x, to_y, c, s], r2.at[h, s, n], 1, place(to_x, to_y, c, z)
            ))
        return one, two

    plan = [steps(p) for p in range(4 * PARTS)]

    def bytes_of(ref, sem):
        pltpu.make_async_copy(ref, ref, sem).wait()

    def core_sum(p):
        half, s = PIECES[p]
        inner = PARTS // 2
        bytes_of(crecv.at[pl.ds(half * inner, inner), s], c_recv.at[p])
        for h in range(half * inner, (half + 1) * inner):
            own = part.at[h, :, :, c, s]
            own[...] = own[...] + crecv[h, s]
            for copy, _, _ in plan[SENDS.index((h, s))][0]:
                copy.start()

    others = partner_ids(x, y, c, z)

    for p in range(8):
        with jax.named_scope(f"density_{p}"):
            density(p)
        if p == EARLY - 1:
            with jax.named_scope("barrier"):
                pl.semaphore_wait(barrier, len(near))
            for q in range(EARLY):
                c_begin(q)
        elif p >= EARLY:
            c_begin(p)
        if p - LAG >= 0 and p >= EARLY:
            with jax.named_scope(f"core_{p}"):
                core_sum(p - LAG)
    with jax.named_scope("core_rest"):
        for p in range(8 - LAG, 8):
            core_sum(p)

    lane = lax.broadcasted_iota(jnp.int32, (8, N), 1)
    sub = lax.broadcasted_iota(jnp.int32, (8, N), 0)

    def fold(value):
        return jnp.sum(value.reshape(16, 8, N), axis=0)

    def products(field, amount):
        rows = jnp.zeros((8, N), f32)
        for j in range(amount):
            line = jnp.sum(fold(field * hres[j]), axis=0, keepdims=True)
            rows = jnp.where(sub == j, line, rows)
        return rows

    def placed(i, rows):
        total = jnp.sum(rows, axis=1, keepdims=True)
        spots = (lane == 8 * i + sub) | (lane == 8 * sub + i)
        return jnp.sum(jnp.where(spots & (sub <= i), total, 0.0), axis=0, keepdims=True)

    def every(start, count=N):
        return pl.ds(start, count, stride=8)

    with jax.named_scope("hist"):
        for i, (a, b) in enumerate(inputs):
            pltpu.make_async_copy(a, b, in_sem.at[i]).wait()
        basis = (tab[0], tab[1])
        for m in range(HIST):
            trial = hin[m] + beta_mix * hres[m]
            hsend[every(m), :] = product(basis, halves(trial - 1.0), ((1,), (1,)))
        row = jnp.zeros((1, N), f32)
        for i in range(HIST):
            row = row + placed(i, products(hres[i], i + 1))
        early_row = row

    def exchange(pairs, source, target, sem):
        for t, slot, _ in pairs:
            pltpu.make_async_remote_copy(
                src_ref=source(t, slot), dst_ref=target,
                send_sem=a_send.at[sem], recv_sem=a_recv.at[sem],
                device_id=t, device_id_type=LOGICAL,
            ).start()

    def arrived(buffer, rows, sem):
        whole = buffer.at[pl.ds(0, 127 * rows)]
        pltpu.make_async_copy(whole, whole, a_recv.at[sem]).wait()

    def sent(buffer, rows, sem):
        whole = buffer.at[pl.ds(0, 127 * rows)]
        pltpu.make_async_copy(whole, whole, a_send.at[sem]).wait()

    def tile(index, rows):
        return pl.ds(pl.multiple_of(index * 8, 8), rows)

    def hist_exchange(pairs):
        exchange(pairs, lambda t, slot: hsend.at[tile(t, 7)], hrecv.at[tile(my_slot, 7)], 0)

    def unheard(o):
        return o[2][0] == 2 and o[2][1] == 2

    hist_order = sorted(others[::-1], key=unheard)
    ends = np.cumsum((0,) + STAGES)
    def hist_stage(h):
        if h == 0:
            hrecv[tile(my_slot, 7), :] = hsend[tile(me, 7), :]
        with jax.named_scope(f"hist_send{h}"):
            if ends[h] <= 29 < ends[h + 1]:
                pl.semaphore_wait(z_sem, 3)
            hist_exchange(hist_order[ends[h] : ends[h + 1]])

    for h in range(PARTS):
        with jax.named_scope(f"step1_{h}"):
            bytes_of(r1.at[h], rs_recv.at[h])
            for p in range(4 * h, 4 * h + 4):
                for _, into, came in plan[p][0]:
                    into[...] = into[...] + came[...]
            if h == 0:
                for e in (1, 2, 3):
                    pl.semaphore_signal(
                        z_sem, inc=1, device_id=place(x, y, c, (z + e) % 4), device_id_type=LOGICAL
                    )
            for p in range(4 * h, 4 * h + 4):
                for copy in plan[p][1]:
                    copy.start()
        hist_stage(h)

    for h in range(PARTS):
        with jax.named_scope(f"step2_{h}"):
            bytes_of(r2.at[h], rs_recv.at[PARTS + h])
            if h == REST_AT:
                hist_exchange(hist_order[ends[-1] :])

    with jax.named_scope("new"):
        blocks = []
        for s in range(4):
            for h in range(PARTS):
                total = part[h, x, y, c, s]
                for n in range(7):
                    total = total + r2[h, s, n]
                blocks.append(total)
        new = jnp.concatenate(blocks, axis=0) - rin[...]
        xsend[every(0), :] = product(basis, halves((rin[...] - 1.0) + beta_mix * new), ((1,), (1,)))
        rows = products(new, HIST)
        rows = jnp.where(sub == 7, jnp.sum(fold(new * new), axis=0, keepdims=True), rows)
        row = early_row + placed(7, rows)
        xsend[every(1), :] = jnp.broadcast_to(row, (N, N))
    with jax.named_scope("x_send"):
        exchange(others, lambda t, slot: xsend.at[tile(t, 2)], xrecv.at[tile(my_slot, 2)], 1)
        xrecv[tile(my_slot, 2), :] = xsend[tile(me, 2), :]
    with jax.named_scope("coulomb"):
        p_index = lax.broadcasted_iota(jnp.int32, (N, N), 0)
        q_index = lax.broadcasted_iota(jnp.int32, (N, N), 1)
        freq_p = jnp.minimum(p_index, N - p_index)
        freq_q = jnp.minimum(q_index, N - q_index)
        freq_r = jnp.minimum(me, N - me)
        squared = freq_p * freq_p + freq_q * freq_q + freq_r * freq_r
        cell = N * spacing
        floored = jnp.maximum(squared, 1).astype(f32)
        coulomb = jnp.where(squared > 0, cell * cell / np.pi / floored, 0.0)

    with jax.named_scope("x_wait"):
        arrived(xrecv, 2, 1)
    with jax.named_scope("hist_wait"):
        arrived(hrecv, 7, 0)

    with jax.named_scope("solve"):
        flat = jnp.sum(xrecv[every(1), :], axis=0, keepdims=True)
        flat = flat * (1.0 / (N * N * N))
        entry = {
            (i, j): jnp.broadcast_to(flat[:, 8 * i + j : 8 * i + j + 1], (8, N))
            for i in range(8) for j in range(i + 1)
        }
        right = [jnp.ones((8, N), f32) for _ in range(8)]
        inverse = []
        for k in range(8):
            inverse.append(1.0 / entry[k, k])
            ratio = {i: entry[i, k] * inverse[k] for i in range(k + 1, 8)}
            for i in range(k + 1, 8):
                right[i] = right[i] - ratio[i] * right[k]
                for j in range(k + 1, i + 1):
                    entry[i, j] = entry[i, j] - ratio[i] * entry[j, k]
            for i in range(k + 1, 8):
                entry[i, k] = ratio[i]
        solved = [right[k] * inverse[k] for k in range(8)]
        for k in range(7, -1, -1):
            for i in range(k):
                solved[i] = solved[i] - entry[k, i] * solved[k]
        total = functools.reduce(lambda a, b: a + b, solved)
        weights = [(value / total)[:1] for value in solved]

    with jax.named_scope("planes"):
        plane = weights[7] * xrecv[every(0), :]
        for m in range(HIST):
            plane = plane + weights[m] * hrecv[every(m), :]
        grouped = jnp.concatenate(regroup([plane[g * 32 : (g + 1) * 32] for g in range(4)]), axis=0)
        second = product(halves(grouped), basis, ((1,), (0,)))
        spectrum = product((tab[2], tab[3]), halves(second), ((1,), (0,))) * coulomb
        back = product((tab[4], tab[5]), halves(spectrum), ((1,), (0,)))
        back = product(halves(back), basis, ((1,), (0,)))
        back = regroup([back[a * 32 : (a + 1) * 32] for a in range(4)])
        vsend[...] = jnp.concatenate(back, axis=0)
    with jax.named_scope("v_send"):
        exchange(others, lambda t, slot: vsend.at[pl.ds(slot, 1)], vrecv.at[pl.ds(me, 1)], 2)
        vrecv[pl.ds(me, 1)] = vsend[pl.ds(my_slot, 1)]

    with jax.named_scope("mix"):
        rho = weights[7] * (rin[...] + beta_mix * new)
        for m in range(HIST):
            rho = rho + weights[m] * (hin[m] + beta_mix * hres[m])
        rho_h[...] = rho
    with jax.named_scope("drain"):
        bytes_of(crecv, r_send.at[0])
        bytes_of(r1, r_send.at[1])
        bytes_of(r2, r_send.at[2])
        sent(hsend, 7, 0)
        sent(xsend, 2, 1)

    with jax.named_scope("v_wait"):
        arrived(vrecv, 1, 2)
    with jax.named_scope("last"):
        v_h[...] = product(halves(vrecv[...].T), basis, ((1,), (0,)))
    sent(vsend, 1, 2)


def local(orbitals, occupations, rho_in, hist_in, hist_res):
    anywhere = pl.BlockSpec(memory_space=pl.ANY)
    vmem, dma = pltpu.VMEM, pltpu.SemaphoreType.DMA
    square = (N, N)
    rho, v = pl.pallas_call(
        kernel,
        out_shape=[pltpu.VMEM(square, f32)] * 2,
        in_specs=[anywhere] * 6,
        out_specs=[pl.BlockSpec(memory_space=pltpu.VMEM)] * 2,
        scratch_shapes=[
            vmem((8, 8, 32, 16, N), bf16), pltpu.SMEM((8,), f32), vmem(square, f32), vmem((HIST, N, N), f32),
            vmem((HIST, N, N), f32), vmem((6, N, N), bf16),
            vmem((PARTS, 4, 4, 2, 4, ROWS, N), f32), vmem((PARTS, 4, 4, 4, ROWS, N), f32),
            vmem((PARTS, 4, 2, 4, ROWS, N), f32), vmem((PARTS, 4, 7, ROWS, N), f32),
            vmem((8 * N, N), f32), vmem((8 * N, N), f32), vmem((8 * N, N), f32),
            vmem((8 * N, N), f32), vmem(square, f32), vmem(square, f32),
            dma((8,)), dma((5,)), dma((8,)), dma((3,)), dma((2 * PARTS,)), dma((3,)), dma((3,)), pltpu.SemaphoreType.REGULAR,
        ],
        compiler_params=pltpu.CompilerParams(
            collective_id=0, has_side_effects=True, vmem_limit_bytes=67043328 - 163840
        ),
    )(
        orbitals.reshape(8, 32, 4, 32, N), occupations, rho_in.reshape(square),
        hist_in.reshape(HIST, N, N), hist_res.reshape(HIST, N, N), tables(),
    )
    return rho.reshape(rho_in.shape), v.reshape(rho_in.shape)


def solution(mesh):
    finer = Mesh(mesh.devices.reshape(4, 4, 2, 4), ("x", "y", "c", "z"))
    in_specs = (
        P(BAND, None, "z", None), P(BAND), P(BAND, "z", None),
        P(None, BAND, "z", None), P(None, BAND, "z", None),
    )
    out_specs = (P(BAND, "z", None), P(BAND, "z", None))
    return jax.shard_map(local, mesh=finer, in_specs=in_specs, out_specs=out_specs, check_vma=False)
```

```python
import functools

import jax
import jax.numpy as jnp
import numpy as np
from jax import lax
from jax.experimental import pallas as pl
from jax.experimental.pallas import tpu as pltpu
from jax.sharding import Mesh
from jax.sharding import PartitionSpec as P

LOGICAL = pl.DeviceIdType.LOGICAL
BAND = ("x", "y", "c")
N = 128
HIST = 7
beta_mix = 0.5
spacing = 0.2
f32 = jnp.float32
bf16 = jnp.bfloat16
STREAMS = (0, 2, 1, 3)
PARTS = 4
ROWS = 32 // PARTS
PIECES = [(h, s) for h in range(2) for s in STREAMS]
SENDS = [(h, s) for h in range(PARTS) for s in STREAMS]
EARLY = 1
LAG = 5
STAGES = (0, 0, 0, 119)
REST_AT = 2


def tables():
    k = np.arange(N)
    angle = 2.0 * np.pi * ((k[:, None] * k[None, :]) % N) / N
    basis = (np.cos(angle) + np.sin(angle)) / np.sqrt(N)
    high = basis.astype(jnp.bfloat16)
    low = (basis - high.astype(np.float64)).astype(jnp.bfloat16).astype(np.float64)
    leak = (high.astype(np.float64) + low)[1:].sum(axis=1)
    low[1:, 0] -= leak
    low[0, 1:] -= leak
    low = low.astype(jnp.bfloat16)
    order = (4 * np.arange(32)[None, :] + np.arange(4)[:, None]).reshape(-1)
    parts = []
    for index in ((slice(None), slice(None)), (slice(None), order), (order, slice(None))):
        parts += [high[index], low[index]]
    return jnp.asarray(np.stack(parts))


def halves(value):
    high = value.astype(bf16)
    return high, (value - high.astype(f32)).astype(bf16)


def product(left, right, dims):
    (k_left,), (k_right,) = dims
    deep = jnp.concatenate(left, axis=k_left)
    tall = jnp.concatenate([right[0], right[0]], axis=k_right)
    dot = functools.partial(
        lax.dot_general, dimension_numbers=(dims, ((), ())), preferred_element_type=f32
    )
    return dot(deep, tall) + dot(left[0], right[1])


def partner_ids(x, y, c, z):
    plane = {(i, j): ((x + i) % 4) * 32 + ((y + j) % 4) * 8 for i in range(4) for j in range(4)}
    rest = {(i, j): ((c + i) % 2) * 4 + (z + j) % 4 for i in range(2) for j in range(4)}
    slot_plane = {(i, j): ((x + i) % 4) * 8 + ((y + j) % 4) * 2 for i in range(4) for j in range(4)}
    slot_rest = {(i, j): ((c + i) % 2) + ((z + j) % 4) * 32 for i in range(2) for j in range(4)}
    moves = [(a, b, d, e) for a in range(4) for b in range(4) for d in range(2) for e in range(4)][1:]

    def hops(m):
        return sum((0, 1, 2, 1)[m[i]] for i in (0, 1, 3))

    moves.sort(key=lambda m: -hops(m))
    return [
        (plane[m[:2]] + rest[m[2:]], slot_plane[m[:2]] + slot_rest[m[2:]], m) for m in moves
    ]


def regroup(rows):
    block = lax.broadcasted_iota(jnp.int32, (32, N), 1) // 32
    turned = {}
    for i in range(4):
        for j in range(4):
            shift = (i - j) % 4
            if (i, shift) not in turned:
                turned[i, shift] = rows[i] if shift == 0 else pltpu.roll(rows[i], 32 * shift, 1)
    out = []
    for j in range(4):
        value = turned[0, (0 - j) % 4]
        for i in range(1, 4):
            value = jnp.where(block == i, turned[i, (i - j) % 4], value)
        out.append(value)
    return out


def kernel(
    orb, occ_h, rin_h, hin_h, hres_h, tab_h, rho_h, v_h,
    orb_v, occ, rin, hin, hres, tab, part, crecv, r1, r2,
    hsend, hrecv, xsend, xrecv, vsend, vrecv,
    load_sem, in_sem, c_recv, r_send, rs_recv, a_send, a_recv, z_sem,
):
    x, y, c, z = (lax.axis_index(a) for a in ("x", "y", "c", "z"))

    def place(px, py, pc, pz):
        return px * 32 + py * 8 + pc * 4 + pz

    me = place(x, y, c, z)
    my_slot = z * 32 + x * 8 + y * 2 + c
    def load(p):
        h, s = PIECES[p]
        return pltpu.make_async_copy(
            orb.at[:, :, s, pl.ds(h * 16, 16)], orb_v.at[p], load_sem.at[p]
        )

    occ_copy = pltpu.make_async_copy(occ_h, occ, in_sem.at[4])
    occ_copy.start()
    load(0).start()
    barrier = pltpu.get_barrier_semaphore()
    near = [place(x, y, 1 - c, z)]
    for e in (2, 1, 3):
        near += [
            place((x + e) % 4, y, c, z), place(x, (y + e) % 4, c, z), place(x, y, c, (z + e) % 4)
        ]
    for t in near:
        pl.semaphore_signal(barrier, inc=1, device_id=t, device_id_type=LOGICAL)
    for p in range(1, 8):
        load(p).start()
    inputs = [(tab_h, tab), (hres_h, hres), (hin_h, hin), (rin_h, rin)]
    for i, (a, b) in enumerate(inputs):
        pltpu.make_async_copy(a, b, in_sem.at[i]).start()

    occ_copy.wait()
    occupied = [occ[k] for k in range(8)]

    def density(p):
        h, s = PIECES[p]
        load(p).wait()

        @pl.loop(0, 4)
        def _(i):
            for row in range(8):
                total = None
                for k in range(8):
                    value = orb_v[p, k, i * 8 + row].astype(f32)
                    term = occupied[k] * (value * value)
                    total = term if total is None else total + term
                for k in range(PARTS // 2):
                    part[h * (PARTS // 2) + k, i, row // 2, row % 2, s] = total[
                        k * ROWS : (k + 1) * ROWS
                    ]

    def c_copy(p):
        h, s = SENDS[p]
        return pltpu.make_async_remote_copy(
            src_ref=part.at[h, :, :, 1 - c, s], dst_ref=crecv.at[h, s],
            send_sem=r_send.at[0], recv_sem=c_recv.at[PIECES.index((h // (PARTS // 2), s))],
            device_id=place(x, y, 1 - c, z), device_id_type=LOGICAL,
        )

    def c_begin(p):
        h, s = PIECES[p]
        for k in range(PARTS // 2):
            c_copy(SENDS.index((h * (PARTS // 2) + k, s))).start()

    flip = {
        "x": {1: x + 1 - 2 * (x % 2), 2: (x + 2) % 4, 3: 3 - x},
        "y": {1: y + 1 - 2 * (y % 2), 2: (y + 2) % 4, 3: 3 - y},
    }
    mine = {"x": x, "y": y}
    orders = {0: ("x", "y", 1), 1: ("x", "y", 3), 2: ("y", "x", 1), 3: ("y", "x", 3)}

    def dev(axis, e):
        if axis == "x":
            return place(flip["x"][e], y, c, z)
        return place(x, flip["y"][e], c, z)

    def steps(p):
        h, s = SENDS[p]
        first, second, e1 = orders[s]
        e2 = 4 - e1

        def remote(src, dst, sem, to):
            return pltpu.make_async_remote_copy(
                src_ref=src, dst_ref=dst, send_sem=r_send.at[1 + sem],
                recv_sem=rs_recv.at[PARTS * sem + h], device_id=to, device_id_type=LOGICAL,
            )

        def rows_of(index):
            if first == "x":
                return part.at[h, index, :, c, s]
            return part.at[h, :, index, c, s]

        def spot(i, j):
            return (i, j) if first == "x" else (j, i)

        one = [
            (remote(rows_of(flip[first][e1]), r1.at[h, s, 0], 0, dev(first, e1)),
             rows_of(mine[first]), r1.at[h, s, 0]),
            (remote(rows_of(flip[first][2]), r1.at[h, s, 1], 0, dev(first, e1)),
             rows_of(flip[first][e2]), r1.at[h, s, 1]),
        ]
        two = []
        moves = [(e2, 2), (e2, 1), (e2, 3), (0, 2), (e2, 0), (0, 1), (0, 3)]
        for n, (i, j) in enumerate(moves):
            to_x, to_y = spot(
                flip[first][i] if i else mine[first], flip[second][j] if j else mine[second]
            )
            two.append(remote(
                part.at[h, to_x, to_y, c, s], r2.at[h, s, n], 1, place(to_x, to_y, c, z)
            ))
        return one, two

    plan = [steps(p) for p in range(4 * PARTS)]

    def bytes_of(ref, sem):
        pltpu.make_async_copy(ref, ref, sem).wait()

    def core_sum(p):
        half, s = PIECES[p]
        inner = PARTS // 2
        bytes_of(crecv.at[pl.ds(half * inner, inner), s], c_recv.at[p])
        for h in range(half * inner, (half + 1) * inner):
            own = part.at[h, :, :, c, s]
            own[...] = own[...] + crecv[h, s]
            for copy, _, _ in plan[SENDS.index((h, s))][0]:
                copy.start()

    others = partner_ids(x, y, c, z)

    for p in range(8):
        with jax.named_scope(f"density_{p}"):
            density(p)
        if p == EARLY - 1:
            with jax.named_scope("barrier"):
                pl.semaphore_wait(barrier, len(near))
            for q in range(EARLY):
                c_begin(q)
        elif p >= EARLY:
            c_begin(p)
        if p - LAG >= 0 and p >= EARLY:
            with jax.named_scope(f"core_{p}"):
                core_sum(p - LAG)
    with jax.named_scope("core_rest"):
        for p in range(8 - LAG, 8):
            core_sum(p)

    lane = lax.broadcasted_iota(jnp.int32, (8, N), 1)
    sub = lax.broadcasted_iota(jnp.int32, (8, N), 0)

    def fold(value):
        return jnp.sum(value.reshape(16, 8, N), axis=0)

    def products(field, amount):
        rows = jnp.zeros((8, N), f32)
        for j in range(amount):
            line = jnp.sum(fold(field * hres[j]), axis=0, keepdims=True)
            rows = jnp.where(sub == j, line, rows)
        return rows

    def placed(i, rows):
        total = jnp.sum(rows, axis=1, keepdims=True)
        spots = (lane == 8 * i + sub) | (lane == 8 * sub + i)
        return jnp.sum(jnp.where(spots & (sub <= i), total, 0.0), axis=0, keepdims=True)

    def every(start, count=N):
        return pl.ds(start, count, stride=8)

    with jax.named_scope("hist"):
        for i, (a, b) in enumerate(inputs):
            pltpu.make_async_copy(a, b, in_sem.at[i]).wait()
        basis = (tab[0], tab[1])
        for m in range(HIST):
            trial = hin[m] + beta_mix * hres[m]
            hsend[every(m), :] = product(basis, halves(trial - 1.0), ((1,), (1,)))
        row = jnp.zeros((1, N), f32)
        for i in range(HIST):
            row = row + placed(i, products(hres[i], i + 1))
        early_row = row

    def exchange(pairs, source, target, sem):
        for t, slot, _ in pairs:
            pltpu.make_async_remote_copy(
                src_ref=source(t, slot), dst_ref=target,
                send_sem=a_send.at[sem], recv_sem=a_recv.at[sem],
                device_id=t, device_id_type=LOGICAL,
            ).start()

    def arrived(buffer, rows, sem):
        whole = buffer.at[pl.ds(0, 127 * rows)]
        pltpu.make_async_copy(whole, whole, a_recv.at[sem]).wait()

    def sent(buffer, rows, sem):
        whole = buffer.at[pl.ds(0, 127 * rows)]
        pltpu.make_async_copy(whole, whole, a_send.at[sem]).wait()

    def tile(index, rows):
        return pl.ds(pl.multiple_of(index * 8, 8), rows)

    def hist_exchange(pairs):
        exchange(pairs, lambda t, slot: hsend.at[tile(t, 7)], hrecv.at[tile(my_slot, 7)], 0)

    def unheard(o):
        return o[2][0] == 2 and o[2][1] == 2

    hist_order = sorted(others[::-1], key=unheard)
    ends = np.cumsum((0,) + STAGES)
    def hist_stage(h):
        if h == 0:
            hrecv[tile(my_slot, 7), :] = hsend[tile(me, 7), :]
        with jax.named_scope(f"hist_send{h}"):
            if ends[h] <= 29 < ends[h + 1]:
                pl.semaphore_wait(z_sem, 3)
            hist_exchange(hist_order[ends[h] : ends[h + 1]])

    for h in range(PARTS):
        with jax.named_scope(f"step1_{h}"):
            bytes_of(r1.at[h], rs_recv.at[h])
            for p in range(4 * h, 4 * h + 4):
                for _, into, came in plan[p][0]:
                    into[...] = into[...] + came[...]
            if h == 0:
                for e in (1, 2, 3):
                    pl.semaphore_signal(
                        z_sem, inc=1, device_id=place(x, y, c, (z + e) % 4), device_id_type=LOGICAL
                    )
            for p in range(4 * h, 4 * h + 4):
                for copy in plan[p][1]:
                    copy.start()
        hist_stage(h)

    for h in range(PARTS):
        with jax.named_scope(f"step2_{h}"):
            bytes_of(r2.at[h], rs_recv.at[PARTS + h])
            if h == REST_AT:
                hist_exchange(hist_order[ends[-1] :])

    with jax.named_scope("new"):
        blocks = []
        for s in range(4):
            for h in range(PARTS):
                total = part[h, x, y, c, s]
                for n in range(7):
                    total = total + r2[h, s, n]
                blocks.append(total)
        new = jnp.concatenate(blocks, axis=0) - rin[...]
        xsend[every(0), :] = product(basis, halves((rin[...] - 1.0) + beta_mix * new), ((1,), (1,)))
        rows = products(new, HIST)
        rows = jnp.where(sub == 7, jnp.sum(fold(new * new), axis=0, keepdims=True), rows)
        row = early_row + placed(7, rows)
        xsend[every(1), :] = jnp.broadcast_to(row, (N, N))
    with jax.named_scope("x_send"):
        exchange(others, lambda t, slot: xsend.at[tile(t, 2)], xrecv.at[tile(my_slot, 2)], 1)
        xrecv[tile(my_slot, 2), :] = xsend[tile(me, 2), :]
    with jax.named_scope("coulomb"):
        p_index = lax.broadcasted_iota(jnp.int32, (N, N), 0)
        q_index = lax.broadcasted_iota(jnp.int32, (N, N), 1)
        freq_p = jnp.minimum(p_index, N - p_index)
        freq_q = jnp.minimum(q_index, N - q_index)
        freq_r = jnp.minimum(me, N - me)
        squared = freq_p * freq_p + freq_q * freq_q + freq_r * freq_r
        cell = N * spacing
        floored = jnp.maximum(squared, 1).astype(f32)
        coulomb = jnp.where(squared > 0, cell * cell / np.pi / floored, 0.0)

    with jax.named_scope("x_wait"):
        arrived(xrecv, 2, 1)
    with jax.named_scope("hist_wait"):
        arrived(hrecv, 7, 0)

    with jax.named_scope("solve"):
        flat = jnp.sum(xrecv[every(1), :], axis=0, keepdims=True)
        flat = flat * (1.0 / (N * N * N))
        entry = {
            (i, j): jnp.broadcast_to(flat[:, 8 * i + j : 8 * i + j + 1], (8, N))
            for i in range(8) for j in range(i + 1)
        }
        right = [jnp.ones((8, N), f32) for _ in range(8)]
        inverse = []
        for k in range(8):
            inverse.append(1.0 / entry[k, k])
            ratio = {i: entry[i, k] * inverse[k] for i in range(k + 1, 8)}
            for i in range(k + 1, 8):
                right[i] = right[i] - ratio[i] * right[k]
                for j in range(k + 1, i + 1):
                    entry[i, j] = entry[i, j] - ratio[i] * entry[j, k]
            for i in range(k + 1, 8):
                entry[i, k] = ratio[i]
        solved = [right[k] * inverse[k] for k in range(8)]
        for k in range(7, -1, -1):
            for i in range(k):
                solved[i] = solved[i] - entry[k, i] * solved[k]
        total = functools.reduce(lambda a, b: a + b, solved)
        weights = [(value / total)[:1] for value in solved]

    with jax.named_scope("planes"):
        plane = weights[7] * xrecv[every(0), :]
        for m in range(HIST):
            plane = plane + weights[m] * hrecv[every(m), :]
        grouped = jnp.concatenate(regroup([plane[g * 32 : (g + 1) * 32] for g in range(4)]), axis=0)
        second = product(halves(grouped), basis, ((1,), (0,)))
        spectrum = product((tab[2], tab[3]), halves(second), ((1,), (0,))) * coulomb
        back = product((tab[4], tab[5]), halves(spectrum), ((1,), (0,)))
        back = product(halves(back), basis, ((1,), (0,)))
        back = regroup([back[a * 32 : (a + 1) * 32] for a in range(4)])
        vsend[...] = jnp.concatenate(back, axis=0)
    with jax.named_scope("v_send"):
        exchange(others, lambda t, slot: vsend.at[pl.ds(slot, 1)], vrecv.at[pl.ds(me, 1)], 2)
        vrecv[pl.ds(me, 1)] = vsend[pl.ds(my_slot, 1)]

    with jax.named_scope("mix"):
        rho = weights[7] * (rin[...] + beta_mix * new)
        for m in range(HIST):
            rho = rho + weights[m] * (hin[m] + beta_mix * hres[m])
        rho_h[...] = rho
    with jax.named_scope("drain"):
        bytes_of(crecv, r_send.at[0])
        bytes_of(r1, r_send.at[1])
        bytes_of(r2, r_send.at[2])
        sent(hsend, 7, 0)
        sent(xsend, 2, 1)

    with jax.named_scope("v_wait"):
        arrived(vrecv, 1, 2)
    with jax.named_scope("last"):
        v_h[...] = product(halves(vrecv[...].T), basis, ((1,), (0,)))
    sent(vsend, 1, 2)


def write_out(rho, v, rho_out, v_out, sem):
    copies = [
        pltpu.make_async_copy(rho, rho_out, sem.at[0]), pltpu.make_async_copy(v, v_out, sem.at[1])
    ]
    for copy in copies:
        copy.start()
    for copy in copies:
        copy.wait()


def local(orbitals, occupations, rho_in, hist_in, hist_res):
    anywhere = pl.BlockSpec(memory_space=pl.ANY)
    vmem, dma = pltpu.VMEM, pltpu.SemaphoreType.DMA
    square = (N, N)
    rho, v = pl.pallas_call(
        kernel,
        out_shape=[pltpu.VMEM(square, f32)] * 2,
        in_specs=[anywhere] * 6,
        out_specs=[pl.BlockSpec(memory_space=pltpu.VMEM)] * 2,
        scratch_shapes=[
            vmem((8, 8, 32, 16, N), bf16), pltpu.SMEM((8,), f32), vmem(square, f32), vmem((HIST, N, N), f32),
            vmem((HIST, N, N), f32), vmem((6, N, N), bf16),
            vmem((PARTS, 4, 4, 2, 4, ROWS, N), f32), vmem((PARTS, 4, 4, 4, ROWS, N), f32),
            vmem((PARTS, 4, 2, 4, ROWS, N), f32), vmem((PARTS, 4, 7, ROWS, N), f32),
            vmem((8 * N, N), f32), vmem((8 * N, N), f32), vmem((8 * N, N), f32),
            vmem((8 * N, N), f32), vmem(square, f32), vmem(square, f32),
            dma((8,)), dma((5,)), dma((8,)), dma((3,)), dma((2 * PARTS,)), dma((3,)), dma((3,)), pltpu.SemaphoreType.REGULAR,
        ],
        compiler_params=pltpu.CompilerParams(
            collective_id=0, has_side_effects=True, vmem_limit_bytes=67043328 - 163840
        ),
    )(
        orbitals.reshape(8, 32, 4, 32, N), occupations, rho_in.reshape(square),
        hist_in.reshape(HIST, N, N), hist_res.reshape(HIST, N, N), tables(),
    )
    rho, v = pl.pallas_call(
        write_out,
        out_shape=[pltpu.HBM(square, f32)] * 2,
        in_specs=[pl.BlockSpec(memory_space=pltpu.VMEM)] * 2,
        out_specs=[anywhere] * 2,
        scratch_shapes=[dma((2,))],
        compiler_params=pltpu.CompilerParams(vmem_limit_bytes=2**20),
    )(rho, v)
    return rho.reshape(rho_in.shape), v.reshape(rho_in.shape)


def solution(mesh):
    finer = Mesh(mesh.devices.reshape(4, 4, 2, 4), ("x", "y", "c", "z"))
    in_specs = (
        P(BAND, None, "z", None), P(BAND), P(BAND, "z", None),
        P(None, BAND, "z", None), P(None, BAND, "z", None),
    )
    out_specs = (P(BAND, "z", None), P(BAND, "z", None))
    return jax.shard_map(local, mesh=finer, in_specs=in_specs, out_specs=out_specs, check_vma=False)
```
